128 devices in a mesh: tp: 128 (over z, y, x, core).
Axes of the slice: x: 4, y: 4, z: 4, core: 2. Of those that a mesh axis runs over, the one named last changes fastest.
Arguments:
- hidden_in: bfloat16 [1, 1024, 2048], P(None, 'tp')
- lengths: int32 [1], replicated
- attn_norm: bfloat16 [2, 2048], replicated
- w_query: bfloat16 [2, 2048, 32, 64], replicated
- w_key: bfloat16 [2, 2048, 32, 64], replicated
- w_value: bfloat16 [2, 2048, 32, 64], replicated
- w_out: bfloat16 [2, 32, 64, 2048], replicated
- mlp_norm: bfloat16 [2, 2048], replicated
- w_gate: bfloat16 [2, 2048, 8192], P(None, None, 'tp')
- w_up: bfloat16 [2, 2048, 8192], P(None, None, 'tp')
- w_down: bfloat16 [2, 8192, 2048], P(None, 'tp')
- final_norm: bfloat16 [2048], replicated
Outputs:
- output: bfloat16 [1, 1024, 2048], P(None, 'tp')
All inputs are finite; a program needn't handle non-finite values.
Results may differ from the reference program's by a relative error of at most 0.0195171.
Values are sent between devices in bfloat16 or wider.
A program may use at most 1 GiB of HBM per device.

```python
import jax
import jax.numpy as jnp
from jax import lax

BATCH = 1
SEQ_DEV = 8
TP_SIZE = 128
SEQ_LEN = 1024
D_MODEL = 2048
HEADS = 32
KV_HEADS = 32
HEAD_DIM = 64
FF_DIM = 8192
LAYERS = 2

NORM_EPS = 1e-5
ROPE_BASE = 500000.0


def setup_inputs(seed: int = 0) -> dict:
    keys = jax.random.split(jax.random.key(seed), 12)
    d_scale = D_MODEL ** -0.5
    hidden_in = jax.random.normal(keys[0], (BATCH, SEQ_LEN, D_MODEL), jnp.float32)
    lengths = jax.random.randint(keys[1], (BATCH,), 1, SEQ_LEN + 1, jnp.int32)
    attn_norm = 1.0 + 0.25 * jax.random.normal(keys[2], (LAYERS, D_MODEL), jnp.float32)
    w_query = 1.4 * d_scale * jax.random.normal(keys[3], (LAYERS, D_MODEL, HEADS, HEAD_DIM), jnp.float32)
    w_key = 1.4 * d_scale * jax.random.normal(keys[4], (LAYERS, D_MODEL, KV_HEADS, HEAD_DIM), jnp.float32)
    w_value = d_scale * jax.random.normal(keys[5], (LAYERS, D_MODEL, KV_HEADS, HEAD_DIM), jnp.float32)
    w_out = (HEADS * HEAD_DIM) ** -0.5 * jax.random.normal(keys[6], (LAYERS, HEADS, HEAD_DIM, D_MODEL), jnp.float32)
    mlp_norm = 1.0 + 0.25 * jax.random.normal(keys[7], (LAYERS, D_MODEL), jnp.float32)
    w_gate = d_scale * jax.random.normal(keys[8], (LAYERS, D_MODEL, FF_DIM), jnp.float32)
    w_up = d_scale * jax.random.normal(keys[9], (LAYERS, D_MODEL, FF_DIM), jnp.float32)
    w_down = FF_DIM ** -0.5 * jax.random.normal(keys[10], (LAYERS, FF_DIM, D_MODEL), jnp.float32)
    final_norm = 1.0 + 0.25 * jax.random.normal(keys[11], (D_MODEL,), jnp.float32)
    return {
        'hidden_in': hidden_in.astype(jnp.bfloat16),
        'lengths': lengths,
        'attn_norm': attn_norm.astype(jnp.bfloat16),
        'w_query': w_query.astype(jnp.bfloat16),
        'w_key': w_key.astype(jnp.bfloat16),
        'w_value': w_value.astype(jnp.bfloat16),
        'w_out': w_out.astype(jnp.bfloat16),
        'mlp_norm': mlp_norm.astype(jnp.bfloat16),
        'w_gate': w_gate.astype(jnp.bfloat16),
        'w_up': w_up.astype(jnp.bfloat16),
        'w_down': w_down.astype(jnp.bfloat16),
        'final_norm': final_norm.astype(jnp.bfloat16),
    }


def rms_norm(hidden, gain):
    h_wide = hidden.astype(jnp.float32)
    inv_rms = lax.rsqrt(jnp.mean(h_wide * h_wide, axis=-1, keepdims=True) + NORM_EPS)
    return (h_wide * inv_rms * gain.astype(jnp.float32)).astype(jnp.bfloat16)


def rotate(proj, cos_tab, sin_tab):
    half_dim = proj.shape[-1] // 2
    first = proj[..., :half_dim]
    second = proj[..., half_dim:]
    return jnp.concatenate([first * cos_tab - second * sin_tab, second * cos_tab + first * sin_tab], axis=-1)


def reference(hidden_in, lengths, attn_norm, w_query, w_key, w_value, w_out, mlp_norm, w_gate, w_up, w_down, final_norm):
    groups = HEADS // KV_HEADS
    ff_shard = FF_DIM // TP_SIZE
    half_dim = HEAD_DIM // 2
    positions = jnp.arange(SEQ_LEN)
    inv_freq = ROPE_BASE ** (-2.0 * jnp.arange(half_dim).astype(jnp.float32) / HEAD_DIM)
    angles = positions.astype(jnp.float32)[:, None, None] * inv_freq[None, None, :]
    cos_tab = jnp.cos(angles)
    sin_tab = jnp.sin(angles)
    score_scale = HEAD_DIM ** -0.5
    key_ok = positions[None, :] < lengths[:, None]

    def layer_fn(hidden, layer_w):
        g_attn, w_q, w_k, w_v, w_o, g_mlp, w_g, w_u, w_d = layer_w
        normed = rms_norm(hidden, g_attn).astype(jnp.float32)
        q_proj = jnp.einsum('bsd,dhe->bshe', normed, w_q.astype(jnp.float32))
        key_proj = jnp.einsum('bsd,dhe->bshe', normed, w_k.astype(jnp.float32))
        v_proj = jnp.einsum('bsd,dhe->bshe', normed, w_v.astype(jnp.float32)).astype(jnp.bfloat16)
        q_rot = rotate(q_proj, cos_tab, sin_tab).astype(jnp.bfloat16)
        k_rot = rotate(key_proj, cos_tab, sin_tab).astype(jnp.bfloat16)
        q_blocks = jnp.moveaxis(q_rot.reshape(BATCH, TP_SIZE, SEQ_DEV, KV_HEADS, groups, HEAD_DIM), 1, 0)
        k_wide = k_rot.astype(jnp.float32)
        v_wide = v_proj.astype(jnp.float32)

        def block_fn(blk_args):
            q_blk, blk_idx = blk_args
            q_pos = blk_idx * SEQ_DEV + jnp.arange(SEQ_DEV)
            scores = jnp.einsum('bqkgd,bskd->bkgqs', q_blk.astype(jnp.float32), k_wide) * score_scale
            allowed = (positions[None, None, :] <= q_pos[None, :, None]) & key_ok[:, None, :]
            scores = jnp.where(allowed[:, None, None, :, :], scores, -1e30)
            prob_mat = jax.nn.softmax(scores, axis=-1).astype(jnp.bfloat16)
            context = jnp.einsum('bkgqs,bskd->bqkgd', prob_mat.astype(jnp.float32), v_wide)
            return context.astype(jnp.bfloat16)

        context = lax.map(block_fn, (q_blocks, jnp.arange(TP_SIZE)))
        context = jnp.moveaxis(context, 0, 1).reshape(BATCH, SEQ_LEN, HEADS, HEAD_DIM)
        attn_out = jnp.einsum('bshe,hed->bsd', context.astype(jnp.float32), w_o.astype(jnp.float32))
        hidden = (hidden.astype(jnp.float32) + attn_out).astype(jnp.bfloat16)
        normed = rms_norm(hidden, g_mlp).reshape(BATCH * SEQ_LEN, D_MODEL)
        wg_shards = jnp.moveaxis(w_g.reshape(D_MODEL, TP_SIZE, ff_shard), 1, 0)
        wu_shards = jnp.moveaxis(w_u.reshape(D_MODEL, TP_SIZE, ff_shard), 1, 0)
        wd_shards = w_d.reshape(TP_SIZE, ff_shard, D_MODEL)

        def shard_fn(acc_sum, shard_w):
            g_w, u_w, d_w = shard_w
            gate_proj = jnp.dot(normed, g_w, preferred_element_type=jnp.float32)
            up_proj = jnp.dot(normed, u_w, preferred_element_type=jnp.float32)
            gated_act = (jax.nn.silu(gate_proj) * up_proj).astype(jnp.bfloat16)
            part_out = jnp.dot(gated_act, d_w, preferred_element_type=jnp.float32).astype(jnp.bfloat16)
            return acc_sum + part_out.astype(jnp.float32), None

        mlp_out, unused = lax.scan(shard_fn, jnp.zeros((BATCH * SEQ_LEN, D_MODEL), jnp.float32), (wg_shards, wu_shards, wd_shards))
        hidden = (hidden.astype(jnp.float32) + mlp_out.reshape(BATCH, SEQ_LEN, D_MODEL)).astype(jnp.bfloat16)
        return hidden, None

    hidden, unused = lax.scan(layer_fn, hidden_in, (attn_norm, w_query, w_key, w_value, w_out, mlp_norm, w_gate, w_up, w_down))
    return rms_norm(hidden, final_norm)
```

```python
import functools

import jax
import jax.numpy as jnp
import numpy as np
from jax import lax
from jax.experimental import pallas as pl
from jax.experimental.pallas import tpu as pltpu
from jax.sharding import PartitionSpec as P

NORM_EPS = 1e-5
ROPE_BASE = 500000.0
MESH = pl.DeviceIdType.MESH
NX, NY, NZ = 4, 4, 4
ROW = 2 * NX
COL = NY * NZ

ROW_STEPS = [(2, 1), (2, 0), (1, 1), (3, 1), (1, 0), (3, 0), (0, 1)]
COL_STEPS = sorted(((dz, dy) for dz in range(NZ) for dy in range(NY) if dz or dy),
                   key=lambda s: -(min(s[0], 4 - s[0]) + min(s[1], 4 - s[1])))


def bf(v):
    return v.astype(jnp.bfloat16)


def f32(v):
    return v.astype(jnp.float32)


def dot_nt(a, b):
    return lax.dot_general(a, b, (((1,), (1,)), ((), ())), preferred_element_type=jnp.float32)


def norm_rows(h, gain):
    inv = lax.rsqrt(jnp.mean(h * h, axis=-1, keepdims=True) + NORM_EPS)
    return h * inv * gain


def kernel(h_ref, len_ref, gattn_ref, gmlp_ref, gfin_ref, freq_ref, wq_ref, wk_ref, wv_ref, wo_ref, wg_ref, wu_ref, wd_ref,
           out_ref,
           hrow, wq_s, wk_s, wv_s, wo_s, wm, kbuf, vbuf, cs, cbuf, hloc, hcol, zs, ps, acts, ysend, ybuf,
           lsem, wosem, msem, asend, arecv, ksend, krecv, vsend, vrecv, csend, crecv, hsend, hrecv, ssend, srecv, gsend, grecv):
    layers = wo_s.shape[0]
    tok, d_model = h_ref.shape
    rtok = ROW * tok
    units = wm.shape[3]
    me = lax.axis_index('tp')
    core = lax.rem(me, 2)
    i = lax.rem(me, ROW)
    x = i // 2
    r = me // ROW
    y = lax.rem(r, NY)
    z = r // NY

    def row_id(dx, dc):
        return 2 * lax.rem(x + dx, NX) + (1 - core if dc else core)

    def row_dev(dx, dc):
        return (r * ROW + row_id(dx, dc),)

    def col_row(dz, dy):
        return NY * lax.rem(z + dz, NZ) + lax.rem(y + dy, NY)

    def col_dev(dz, dy):
        return (col_row(dz, dy) * ROW + i,)

    def send(src, dst, ssem, rsem, dev):
        pltpu.make_async_remote_copy(src_ref=src, dst_ref=dst, send_sem=ssem, recv_sem=rsem, device_id=dev,
                                     device_id_type=MESH).start()

    def wait(ref, sem):
        pltpu.make_async_copy(ref, ref, sem).wait()

    heads = 4
    half = 32
    local = []

    def load(src, dst, sem):
        c = pltpu.make_async_copy(src, dst, sem)
        c.start()
        return c

    def load_qkv(l):
        base = i * (2 * heads * half)
        got = []
        for k, (src, dst) in enumerate(((wq_ref, wq_s), (wk_ref, wk_s))):
            for j in range(heads):
                for s in range(2):
                    got.append(load(src.at[l, pl.ds(base + (2 * j + s) * half, half)],
                                    dst.at[l, pl.ds((s * heads + j) * half, half)], lsem.at[l, 9 * k + 2 * j + s]))
        got.append(load(wv_ref.at[l, pl.ds(base, 2 * heads * half)], wv_s.at[l], lsem.at[l, 8]))
        return got

    def load_mlp(l):
        return [load(w.at[l], wm.at[l, i, k], msem.at[l, k]) for k, w in enumerate((wg_ref, wu_ref, wd_ref))]

    qkv_loads = [load_qkv(0)]
    mlp_loads = [load_mlp(0), load_mlp(1)]
    wo_loads = [load(wo_ref.at[0], wo_s.at[0], wosem.at[0])]
    qkv_loads.append(load_qkv(1))
    wo_loads.append(load(wo_ref.at[1], wo_s.at[1], wosem.at[1]))

    kbuf[...] = jnp.zeros_like(kbuf)
    vbuf[...] = jnp.zeros_like(vbuf)
    barrier = pltpu.get_barrier_semaphore()
    for s in ROW_STEPS:
        pl.semaphore_signal(barrier, inc=1, device_id=row_dev(*s), device_id_type=MESH)
    for s in COL_STEPS:
        pl.semaphore_signal(barrier, inc=1, device_id=col_dev(*s), device_id_type=MESH)
    hrow[pl.ds(i, 1)] = h_ref[...][None]
    pos = f32(r * rtok + lax.broadcasted_iota(jnp.int32, (rtok, 1), 0))
    angles = pos * freq_ref[...]
    cos_tab = jnp.cos(angles)
    sin_tab = jnp.sin(angles)
    pl.semaphore_wait(barrier, len(ROW_STEPS) + len(COL_STEPS))

    def slot(dx, dc):
        return row_id((dx + NX) % NX, dc)

    hu = units // 2

    def g_send(l):
        for c in mlp_loads[l]:
            c.wait()
        own = wm.at[l, i]
        send(own, own, gsend.at[l, 1], grecv.at[l, 1], row_dev(1, 0))
        send(own, own, gsend.at[l, 2], grecv.at[l, 2], row_dev(3, 0))
        send(own, own, gsend.at[l, 0], grecv.at[l, 0], row_dev(0, 1))

    def g_fwd(l):
        a = wm.at[l, slot(-1, 0)]
        ah = wm.at[l, slot(-1, 0), :, pl.ds(0, hu)]
        b = wm.at[l, slot(1, 0)]
        bh = wm.at[l, slot(1, 0), :, pl.ds(hu, hu)]
        wait(a, grecv.at[l, 1])
        send(ah, ah, gsend.at[l, 3], grecv.at[l, 3], row_dev(1, 0))
        wait(b, grecv.at[l, 2])
        send(bh, bh, gsend.at[l, 4], grecv.at[l, 4], row_dev(3, 0))
        send(a, a, gsend.at[l, 5], grecv.at[l, 5], row_dev(0, 1))
        send(b, b, gsend.at[l, 6], grecv.at[l, 6], row_dev(0, 1))

    def g_halves(l, dc):
        s = slot(2, dc)
        return wm.at[l, s, :, pl.ds(0, hu)], wm.at[l, s, :, pl.ds(hu, hu)]

    def g_fwd2(l):
        for k, ref in enumerate(g_halves(l, 0)):
            wait(ref, grecv.at[l, 3 + k])
            send(ref, ref, gsend.at[l, 7 + k], grecv.at[l, 7 + k], row_dev(0, 1))

    def g_done(l):
        wait(wm.at[l, slot(0, 1)], grecv.at[l, 0])
        wait(wm.at[l, slot(-1, 1)], grecv.at[l, 5])
        wait(wm.at[l, slot(1, 1)], grecv.at[l, 6])
        for k, ref in enumerate(g_halves(l, 1)):
            wait(ref, grecv.at[l, 7 + k])
        for k in (0, 1, 2, 5, 6):
            wait(wm.at[l, i], gsend.at[l, k])
        for k in (3, 4, 7, 8):
            wait(wm.at[l, i, :, pl.ds(0, hu)], gsend.at[l, k])

    lane = lax.broadcasted_iota(jnp.int32, (1, 2 * heads * half), 1)
    length = len_ref[0]

    hidden = f32(h_ref[...])
    for l in range(layers):
        g_attn = f32(gattn_ref[...])[l:l + 1]
        g_mlp = f32(gmlp_ref[...])[l:l + 1]
        own = h_ref if l == 0 else hloc.at[0]
        for k, s in enumerate(ROW_STEPS):
            send(own, hrow.at[i], asend.at[k], arecv.at[k], row_dev(*s))
        for k, (dx, dc) in enumerate(ROW_STEPS):
            wait(hrow.at[slot(-dx, dc)], arecv.at[k])
        if l == 0:
            g_send(0)
        else:
            g_fwd(1)
        zrow = bf(norm_rows(f32(hrow[...]).reshape(rtok, d_model), g_attn))
        zs[0:rtok] = zrow
        for c in qkv_loads[l]:
            c.wait()

        def rotated(w):
            p = dot_nt(zs[0:rtok], w)
            a, b = p[:, :heads * half], p[:, heads * half:]
            return bf(jnp.concatenate([a * cos_tab - b * sin_tab, b * cos_tab + a * sin_tab], axis=1))

        kbuf[pl.ds(r, 1)] = rotated(wk_s[l])[None]
        vbuf[pl.ds(r, 1)] = bf(dot_nt(zs[0:rtok], wv_s[l]))[None]
        for k, (dz, dy) in enumerate(COL_STEPS):
            to = col_row(dz, dy)

            @pl.when(to > r)
            def _():
                send(kbuf.at[r], kbuf.at[r], ksend.at[k], krecv.at[k], col_dev(dz, dy))
                send(vbuf.at[r], vbuf.at[r], vsend.at[k], vrecv.at[k], col_dev(dz, dy))

        q_rot = rotated(wq_s[l])
        q_all = jnp.concatenate(
            [jnp.where(lax.rem(lane, heads * half) // half == j, q_rot, jnp.zeros_like(q_rot)) for j in range(heads)], axis=0)
        for k, (dz, dy) in enumerate(COL_STEPS):
            frm = col_row(NZ - dz, NY - dy)

            @pl.when(frm < r)
            def _():
                wait(kbuf.at[frm], krecv.at[k])
                wait(vbuf.at[frm], vrecv.at[k])

        keys = kbuf.shape[0] * rtok
        scores = dot_nt(q_all, kbuf[...].reshape(keys, 2 * heads * half)) * (2 * half) ** -0.5
        k_pos = lax.broadcasted_iota(jnp.int32, scores.shape, 1)
        q_pos = r * rtok + lax.rem(lax.broadcasted_iota(jnp.int32, scores.shape, 0), rtok)
        scores = jnp.where((k_pos <= q_pos) & (k_pos < length), scores, -1e30)
        e = jnp.exp(scores - jnp.max(scores, axis=-1, keepdims=True))
        probs = bf(e * (1.0 / jnp.sum(e, axis=-1, keepdims=True)))
        pv = jnp.dot(probs, vbuf[...].reshape(keys, 2 * heads * half), preferred_element_type=jnp.float32)
        ctx = jnp.zeros((rtok, 2 * heads * half), jnp.float32)
        for j in range(heads):
            ctx = jnp.where(lane // (2 * half) == j, pv[j * rtok:(j + 1) * rtok], ctx)
        cs[...] = bf(ctx.reshape(ROW, tok, 2 * heads * half))
        for k, s in enumerate(ROW_STEPS):
            send(cs.at[row_id(*s)], cbuf.at[i], csend.at[k], crecv.at[k], row_dev(*s))
        cbuf[pl.ds(i, 1)] = cs[pl.ds(i, 1)]
        wo_loads[l].wait()
        for k, (dx, dc) in enumerate(ROW_STEPS):
            wait(cbuf.at[slot(-dx, dc)], crecv.at[k])
        if l == 0:
            g_fwd(0)
            g_send(1)
        ctx_all = jnp.concatenate([cbuf[k] for k in range(ROW)], axis=1)
        attn_out = jnp.dot(ctx_all, wo_s[l], preferred_element_type=jnp.float32)
        hid_b = bf(hidden + attn_out)
        hidden = f32(hid_b)
        hloc[1] = hid_b
        hcol[0] = hid_b
        for k, s in enumerate(COL_STEPS):
            send(hloc.at[1], hcol.at[k + 1], hsend.at[k], hrecv.at[k], col_dev(*s))
        g_fwd2(l)
        for k in range(COL - 1):
            wait(hcol.at[k + 1], hrecv.at[k])
        zs[...] = bf(norm_rows(f32(hcol[...]).reshape(COL * tok, d_model), g_mlp))
        g_done(l)
        grp = ROW // 2
        for b in range(2):
            gate = dot_nt(zs[...], wm[l, b * grp:(b + 1) * grp, 0].reshape(grp * units, d_model))
            up = dot_nt(zs[...], wm[l, b * grp:(b + 1) * grp, 1].reshape(grp * units, d_model))
            act = bf(gate * (1.0 / (1.0 + jnp.exp(-gate))) * up)
            for j in range(grp):
                acts[b, j * COL * tok:(j + 1) * COL * tok] = jnp.where(lane // units == j, act, jnp.zeros_like(act))
        parts = 4
        width = d_model // parts
        for n in range(parts):
            cols = slice(n * width, (n + 1) * width)
            total = jnp.zeros((COL * tok, width), jnp.float32)
            for b in range(2):
                wd = wm[l, b * grp:(b + 1) * grp, 2, :, cols].reshape(grp * units, width)
                prod = jnp.dot(acts[b], wd, preferred_element_type=jnp.float32)
                for j in range(grp):
                    total = total + f32(bf(prod[j * COL * tok:(j + 1) * COL * tok]))
            ysend[:, :, cols] = total.reshape(COL, tok, width)
            for k, (dz, dy) in enumerate(COL_STEPS):
                send(ysend.at[k + 1, :, cols], ybuf.at[k, :, cols], ssend.at[k], srecv.at[k], col_dev(NZ - dz, NY - dy))
        total = ysend[0]
        for k in range(COL - 1):
            wait(ybuf.at[k], srecv.at[k])
            total = total + ybuf[k]
        hid_b = bf(hidden + total)
        hidden = f32(hid_b)
        for k in range(ROW - 1):
            wait(own, asend.at[k])
            wait(cs.at[0], csend.at[k])
        for k, (dz, dy) in enumerate(COL_STEPS):
            @pl.when(col_row(dz, dy) > r)
            def _():
                wait(kbuf.at[r], ksend.at[k])
                wait(vbuf.at[r], vsend.at[k])
            wait(hloc.at[1], hsend.at[k])
            wait(ysend.at[0], ssend.at[k])
        if l < layers - 1:
            hloc[0] = hid_b
            hrow[pl.ds(i, 1)] = hid_b[None]
    out_ref[...] = bf(norm_rows(hidden, f32(gfin_ref[...])))


def solution(mesh):
    def device_fn(hidden_in, lengths, attn_norm, w_query, w_key, w_value, w_out, mlp_norm, w_gate, w_up, w_down, final_norm):
        batch, tok, d_model = hidden_in.shape
        layers, _, heads, head_dim = w_query.shape
        units = w_gate.shape[2]
        half = head_dim // 2
        freq = ROPE_BASE ** (-2.0 * np.arange(half, dtype=np.float32) / head_dim)
        freq = jnp.asarray(np.tile(freq.astype(np.float32), heads // ROW)[None])

        def by_rows(w):
            return jnp.transpose(w, (0, 2, 3, 1)).reshape(layers, heads * head_dim, d_model)

        wide = heads * head_dim // ROW
        dma = pltpu.SemaphoreType.DMA
        b16 = jnp.bfloat16
        vm = pl.BlockSpec(memory_space=pltpu.VMEM)
        hbm = pl.BlockSpec(memory_space=pl.ANY)
        rtok = ROW * tok
        out = pl.pallas_call(
            kernel,
            name='prefill',
            out_shape=jax.ShapeDtypeStruct((tok, d_model), b16),
            in_specs=[vm, pl.BlockSpec(memory_space=pltpu.SMEM), vm, vm, vm, vm] + [hbm] * 7,
            out_specs=vm,
            scratch_shapes=[
                pltpu.VMEM((ROW, tok, d_model), b16),
                pltpu.VMEM((layers, wide, d_model), b16),
                pltpu.VMEM((layers, wide, d_model), b16),
                pltpu.VMEM((layers, wide, d_model), b16),
                pltpu.VMEM((layers, heads * head_dim, d_model), b16),
                pltpu.VMEM((layers, ROW, 3, units, d_model), b16),
                pltpu.VMEM((COL, rtok, wide), b16),
                pltpu.VMEM((COL, rtok, wide), b16),
                pltpu.VMEM((ROW, tok, wide), b16),
                pltpu.VMEM((ROW, tok, wide), b16),
                pltpu.VMEM((2, tok, d_model), b16),
                pltpu.VMEM((COL, tok, d_model), b16),
                pltpu.VMEM((COL * tok, d_model), b16),
                pltpu.VMEM((8, 128), b16),
                pltpu.VMEM((2, ROW // 2 * COL * tok, ROW // 2 * units), b16),
                pltpu.VMEM((COL, tok, d_model), jnp.float32),
                pltpu.VMEM((COL - 1, tok, d_model), jnp.float32),
                dma((layers, 18)), dma((layers,)), dma((layers, 3)),
                dma((ROW - 1,)), dma((ROW - 1,)),
                dma((COL - 1,)), dma((COL - 1,)), dma((COL - 1,)), dma((COL - 1,)),
                dma((ROW - 1,)), dma((ROW - 1,)),
                dma((COL - 1,)), dma((COL - 1,)),
                dma((COL - 1,)), dma((COL - 1,)),
                dma((layers, 9)), dma((layers, 9)),
            ],
            compiler_params=pltpu.CompilerParams(collective_id=0, has_side_effects=True, vmem_limit_bytes=60 * 1024 * 1024),
        )(hidden_in.reshape(tok, d_model), lengths, attn_norm, mlp_norm, final_norm.reshape(1, d_model), freq,
          by_rows(w_query), by_rows(w_key), by_rows(w_value), w_out.reshape(layers, heads * head_dim, d_model),
          jnp.transpose(w_gate, (0, 2, 1)), jnp.transpose(w_up, (0, 2, 1)), w_down)
        return out.reshape(batch, tok, d_model)

    seq_part = P(None, 'tp', None)
    in_specs = (seq_part, P(), P(), P(), P(), P(), P(), P(), P(None, None, 'tp'), P(None, None, 'tp'), P(None, 'tp', None), P())
    return jax.shard_map(device_fn, mesh=mesh, in_specs=in_specs, out_specs=seq_part, check_vma=False)
```

```python
import functools

import jax
import jax.numpy as jnp
import numpy as np
from jax import lax
from jax.experimental import pallas as pl
from jax.experimental.pallas import tpu as pltpu
from jax.sharding import PartitionSpec as P

NORM_EPS = 1e-5
ROPE_BASE = 500000.0
MESH = pl.DeviceIdType.MESH
NX, NY, NZ = 4, 4, 4
ROW = 2 * NX
COL = NY * NZ

ROW_STEPS = [(2, 1), (2, 0), (1, 1), (3, 1), (1, 0), (3, 0), (0, 1)]
COL_STEPS = sorted(((dz, dy) for dz in range(NZ) for dy in range(NY) if dz or dy),
                   key=lambda s: -(min(s[0], 4 - s[0]) + min(s[1], 4 - s[1])))
PLANE_STEPS = sorted(((dy, dx, dc) for dy in range(NY) for dx in range(NX) for dc in range(2) if dy or dx or dc),
                     key=lambda s: -(min(s[0], 4 - s[0]) + min(s[1], 4 - s[1])))


class Phases:
    def __init__(self):
        self.open = None

    def __call__(self, name=None):
        if self.open is not None:
            self.open.__exit__(None, None, None)
        self.open = jax.named_scope(name) if name else None
        if name:
            self.open.__enter__()


def bf(v):
    return v.astype(jnp.bfloat16)


def f32(v):
    return v.astype(jnp.float32)


def dot_nt(a, b):
    return lax.dot_general(a, b, (((1,), (1,)), ((), ())), preferred_element_type=jnp.float32)


def norm_rows(h, gain):
    inv = lax.rsqrt(jnp.mean(h * h, axis=-1, keepdims=True) + NORM_EPS)
    return h * inv * gain


def kernel(h_ref, len_ref, gattn_ref, gmlp_ref, gfin_ref, freq_ref, wq_ref, wk_ref, wv_ref, wo_ref, wg_ref, wu_ref, wd_ref,
           out_ref,
           hrow, wq_s, wkv_s, wo_s, wm, kvs, kvbuf, qs, qbuf, cs, cbuf, hloc, hcol, zs, acts, ysend, ybuf,
           lsem, wosem, msem, asend, arecv, kvsend, kvrecv, qsend, qrecv, csend, crecv, hsend, hrecv, ssend, srecv, gsend, grecv):
    phase = Phases()
    phase('start')
    layers = wo_s.shape[0]
    tok, d_model = h_ref.shape
    rtok = ROW * tok
    heads, wide = kvs.shape[0], kvs.shape[2]
    hd = wide // 2
    half = hd // 2
    units = wm.shape[3]
    me = lax.axis_index('tp')
    core = lax.rem(me, 2)
    i = lax.rem(me, ROW)
    x = i // 2
    r = me // ROW
    y = lax.rem(r, NY)
    z = r // NY

    def row_id(dx, dc):
        return 2 * lax.rem(x + (dx + NX) % NX, NX) + (1 - core if dc else core)

    def row_dev(dx, dc):
        return (r * ROW + row_id(dx, dc),)

    def y_at(dy):
        return lax.rem(y + (dy + NY) % NY, NY)

    def plane_dev(dy, dx, dc):
        return ((z * NY + y_at(dy)) * ROW + row_id(dx, dc),)

    def col_dev(dz, dy):
        return ((NY * lax.rem(z + (dz + NZ) % NZ, NZ) + y_at(dy)) * ROW + i,)

    def send(src, dst, ssem, rsem, dev):
        pltpu.make_async_remote_copy(src_ref=src, dst_ref=dst, send_sem=ssem, recv_sem=rsem, device_id=dev,
                                     device_id_type=MESH).start()

    def wait(ref, sem):
        pltpu.make_async_copy(ref, ref, sem).wait()

    def load(src, dst, sem):
        c = pltpu.make_async_copy(src, dst, sem)
        c.start()
        return c

    def load_qkv(l):
        base = i * (heads * hd)
        got = []
        for j in range(heads):
            rows = pl.ds(base + j * hd, hd)
            got.append(load(wk_ref.at[l, rows], wkv_s.at[l, j, 0:hd], lsem.at[l, 2 * j]))
            got.append(load(wv_ref.at[l, rows], wkv_s.at[l, j, hd:wide], lsem.at[l, 2 * j + 1]))
        got.append(load(wq_ref.at[l, pl.ds(base, heads * hd)], wq_s.at[l], lsem.at[l, 2 * heads]))
        return got

    def load_mlp(l):
        return [load(w.at[l], wm.at[l, i, k], msem.at[l, k]) for k, w in enumerate((wg_ref, wu_ref, wd_ref))]

    mlp_loads = [load_mlp(0)]
    qkv_loads = [load_qkv(0)]
    wo_loads = [load(wo_ref.at[0], wo_s.at[0], wosem.at[0])]
    mlp_loads.append(load_mlp(1))
    qkv_loads.append(load_qkv(1))
    wo_loads.append(load(wo_ref.at[1], wo_s.at[1], wosem.at[1]))

    kvbuf[...] = jnp.zeros_like(kvbuf)
    barrier = pltpu.get_barrier_semaphore()
    partners = [plane_dev(*s) for s in PLANE_STEPS] + [col_dev(*s) for s in COL_STEPS if s[0]]
    for dev in partners:
        pl.semaphore_signal(barrier, inc=1, device_id=dev, device_id_type=MESH)
    hrow[pl.ds(i, 1)] = h_ref[...][None]
    lane = lax.broadcasted_iota(jnp.int32, (1, wide), 1)
    pos = f32(r * rtok + lax.broadcasted_iota(jnp.int32, (rtok, 1), 0))
    angles = pos * freq_ref[...]
    cos_tab = jnp.cos(angles)
    sin_tab = jnp.sin(angles)
    sin_tab = jnp.where(lax.rem(lane, hd) < half, -sin_tab, sin_tab)
    phase('barrier')
    pl.semaphore_wait(barrier, len(partners))

    hu = units // 2
    spans = (pl.ds(0, 2), pl.ds(2, 1))
    low, high = pl.ds(0, hu), pl.ds(hu, hu)

    def blk(l, p, dx, dc, rows=None):
        if rows is None:
            return wm.at[l, row_id(dx, dc), spans[p]]
        return wm.at[l, row_id(dx, dc), spans[p], rows]

    def g_push(l, p, k, ref, dx, dc):
        send(ref, ref, gsend.at[l, p, k], grecv.at[l, p, k], row_dev(dx, dc))

    def g_send(l, p):
        for c in (mlp_loads[l][:2], mlp_loads[l][2:])[p]:
            c.wait()
        own = blk(l, p, 0, 0)
        g_push(l, p, 1, own, 1, 0)
        g_push(l, p, 2, own, -1, 0)
        g_push(l, p, 0, own, 0, 1)

    def g_fwd(l, p):
        wait(blk(l, p, -1, 0), grecv.at[l, p, 1])
        g_push(l, p, 3, blk(l, p, -1, 0, low), 1, 0)
        wait(blk(l, p, 1, 0), grecv.at[l, p, 2])
        g_push(l, p, 4, blk(l, p, 1, 0, high), -1, 0)
        g_push(l, p, 5, blk(l, p, -1, 0), 0, 1)
        g_push(l, p, 6, blk(l, p, 1, 0), 0, 1)

    def g_fwd2(l, p):
        for k, rows in enumerate((low, high)):
            wait(blk(l, p, 2, 0, rows), grecv.at[l, p, 3 + k])
            g_push(l, p, 7 + k, blk(l, p, 2, 0, rows), 0, 1)

    def g_done(l, p):
        wait(blk(l, p, 0, 1), grecv.at[l, p, 0])
        wait(blk(l, p, -1, 1), grecv.at[l, p, 5])
        wait(blk(l, p, 1, 1), grecv.at[l, p, 6])
        for k, rows in enumerate((low, high)):
            wait(blk(l, p, 2, 1, rows), grecv.at[l, p, 7 + k])

    def g_drain(l, p):
        for k in (0, 1, 2, 5, 6):
            wait(blk(l, p, 0, 0), gsend.at[l, p, k])
        for k in (3, 4, 7, 8):
            wait(blk(l, p, 0, 0, low), gsend.at[l, p, k])

    length = len_ref[0]

    def turned(p, c, s):
        swapped = jnp.where(lax.rem(lane, hd) < half, pltpu.roll(p, wide - half, 1), pltpu.roll(p, half, 1))
        return p * c + swapped * s

    hidden = f32(h_ref[...])
    for l in range(layers):
        g_attn = f32(gattn_ref[...])[l:l + 1]
        g_mlp = f32(gmlp_ref[...])[l:l + 1]
        phase(f'row_h#l={l}')
        own = h_ref if l == 0 else hloc.at[0]
        for k, s in enumerate(ROW_STEPS):
            send(own, hrow.at[i], asend.at[k], arecv.at[k], row_dev(*s))
        if l == 0:
            g_send(0, 0)
        for k, (dx, dc) in enumerate(ROW_STEPS):
            wait(hrow.at[row_id(-dx, dc)], arecv.at[k])
        phase(f'qkv#l={l}')
        zs[0:rtok] = bf(norm_rows(f32(hrow[...]).reshape(rtok, d_model), g_attn))
        for c in qkv_loads[l]:
            c.wait()
        kv = dot_nt(zs[0:rtok], wkv_s[l].reshape(heads * wide, d_model))
        for j in range(heads):
            p = kv[:, j * wide:(j + 1) * wide]
            kvs[j] = bf(jnp.where(lane < hd, turned(p, cos_tab, sin_tab), p))
        for dz in (3, 2, 1, 0):
            @pl.when(z + dz < NZ)
            def _():
                for dy in (2, 1, 3, 0):
                    if dz or dy:
                        send(kvs.at[y_at(dy)], kvbuf.at[r], kvsend.at[dz, dy], kvrecv.at[dz, dy], col_dev(dz, dy))
        kvbuf[pl.ds(r, 1)] = kvs[pl.ds(y, 1)]
        q = dot_nt(zs[0:rtok], wq_s[l])
        for j in range(0, heads, 2):
            pair = turned(q[:, j * hd:(j + 2) * hd], cos_tab, sin_tab)
            qs[j] = bf(jnp.where(lane < hd, pair, 0.0))
            qs[j + 1] = bf(jnp.where(lane < hd, pltpu.roll(pair, hd, 1), 0.0))
        for dy in (2, 1, 3):
            send(qs.at[y_at(dy)], qbuf.at[y], qsend.at[dy], qrecv.at[dy], col_dev(0, dy))
        qbuf[pl.ds(y, 1)] = qs[pl.ds(y, 1)]
        phase(f'kv_wait#l={l}')
        for dy in (1, 3, 2):
            wait(qbuf.at[y_at(-dy)], qrecv.at[dy])
        for dz in range(NZ):
            @pl.when(z - dz >= 0)
            def _():
                for dy in range(NY):
                    if dz or dy:
                        wait(kvbuf.at[(z - dz) * NY + y_at(-dy)], kvrecv.at[dz, dy])
        phase(f'attn#l={l}')
        keys = COL * rtok
        quer = NY * rtok
        kv_all = kvbuf[...].reshape(keys, wide)
        scores = dot_nt(qbuf[...].reshape(quer, wide), kv_all) * hd ** -0.5
        k_pos = lax.broadcasted_iota(jnp.int32, scores.shape, 1)
        q_pos = z * quer + lax.broadcasted_iota(jnp.int32, scores.shape, 0)
        scores = jnp.where((k_pos <= q_pos) & (k_pos < length), scores, -1e30)
        e = jnp.exp(scores - jnp.max(scores, axis=-1, keepdims=True))
        probs = bf(e * (1.0 / jnp.sum(e, axis=-1, keepdims=True)))
        pv = jnp.dot(probs, kv_all, preferred_element_type=jnp.float32)
        ctx = jnp.where(lax.rem(y, 2) == 0, pltpu.roll(pv, hd, 1), pv)
        cs[...] = bf(ctx.reshape(NY * ROW, tok, wide))
        phase(f'ctx#l={l}')
        slot = ROW * y + i
        for k, (dy, dx, dc) in enumerate(PLANE_STEPS):
            send(cs.at[ROW * y_at(dy) + row_id(dx, dc)], cbuf.at[slot], csend.at[k], crecv.at[k], plane_dev(dy, dx, dc))
        cbuf[pl.ds(slot, 1)] = cs[pl.ds(slot, 1)]
        phase(f'g_b#l={l}')
        if l == 0:
            g_fwd(0, 0)
            g_send(0, 1)
        else:
            g_fwd(1, 1)
            g_fwd2(1, 0)
        wo_loads[l].wait()
        phase(f'ctx_wait#l={l}')
        for k, (dy, dx, dc) in enumerate(PLANE_STEPS):
            wait(cbuf.at[ROW * y_at(-dy) + row_id(-dx, dc)], crecv.at[k])
        phase(f'out#l={l}')
        pieces = []
        for k in range(ROW):
            for j in range(0, heads, 2):
                pieces.append(jnp.where(lane < hd, cbuf[j * ROW + k], cbuf[(j + 1) * ROW + k]))
        ctx_all = jnp.concatenate(pieces, axis=1)
        attn_out = jnp.dot(ctx_all, wo_s[l], preferred_element_type=jnp.float32)
        hid_b = bf(hidden + attn_out)
        hidden = f32(hid_b)
        hloc[1] = hid_b
        hcol[0] = hid_b
        phase(f'col_h#l={l}')
        for k, s in enumerate(COL_STEPS):
            send(hloc.at[1], hcol.at[k + 1], hsend.at[k], hrecv.at[k], col_dev(*s))
        if l == 0:
            g_fwd(0, 1)
            g_fwd2(0, 0)
        else:
            g_fwd2(1, 1)
        phase(f'col_h_wait#l={l}')
        for k in range(COL - 1):
            wait(hcol.at[k + 1], hrecv.at[k])
        zs[...] = bf(norm_rows(f32(hcol[...]).reshape(COL * tok, d_model), g_mlp))
        phase(f'g_done#l={l}')
        g_done(l, 0)
        phase(f'mlp_up#l={l}')
        grp = ROW // 2
        ulane = lax.broadcasted_iota(jnp.int32, (1, grp * units), 1) // units
        for b in range(2):
            gate = dot_nt(zs[...], wm[l, b * grp:(b + 1) * grp, 0].reshape(grp * units, d_model))
            up = dot_nt(zs[...], wm[l, b * grp:(b + 1) * grp, 1].reshape(grp * units, d_model))
            act = bf(gate * (1.0 / (1.0 + jnp.exp(-gate))) * up)
            for j in range(grp):
                acts[b, j * COL * tok:(j + 1) * COL * tok] = jnp.where(ulane == j, act, jnp.zeros_like(act))
        phase(f'g_done2#l={l}')
        if l == 0:
            g_fwd2(0, 1)
            g_send(1, 0)
            g_send(1, 1)
        g_done(l, 1)
        phase(f'mlp_down#l={l}')
        parts = 4
        width = d_model // parts
        for n in range(parts):
            cols = slice(n * width, (n + 1) * width)
            total = jnp.zeros((COL * tok, width), jnp.float32)
            for b in range(2):
                wd = wm[l, b * grp:(b + 1) * grp, 2, :, cols].reshape(grp * units, width)
                prod = jnp.dot(acts[b], wd, preferred_element_type=jnp.float32)
                for j in range(grp):
                    total = total + f32(bf(prod[j * COL * tok:(j + 1) * COL * tok]))
            ysend[:, :, cols] = total.reshape(COL, tok, width)
            for k, (dz, dy) in enumerate(COL_STEPS):
                send(ysend.at[k + 1, :, cols], ybuf.at[k, :, cols], ssend.at[k], srecv.at[k], col_dev(-dz, -dy))
        phase(f'rs_wait#l={l}')
        if l == 0:
            g_fwd(1, 0)
        total = ysend[0]
        for k in range(COL - 1):
            wait(ybuf.at[k], srecv.at[k])
            total = total + ybuf[k]
        hid_b = bf(hidden + total)
        hidden = f32(hid_b)
        phase(f'drain#l={l}')
        for k in range(ROW - 1):
            wait(own, asend.at[k])
        for k in range(len(PLANE_STEPS)):
            wait(cs.at[0], csend.at[k])
        for dz in range(NZ):
            @pl.when(z + dz < NZ)
            def _():
                for dy in range(NY):
                    if dz or dy:
                        wait(kvs.at[0], kvsend.at[dz, dy])
        for dy in (1, 2, 3):
            wait(qs.at[0], qsend.at[dy])
        for k in range(COL - 1):
            wait(hloc.at[1], hsend.at[k])
            wait(ysend.at[0], ssend.at[k])
        if l < layers - 1:
            hloc[0] = hid_b
            hrow[pl.ds(i, 1)] = hid_b[None]
    phase('end')
    for l in range(layers):
        g_drain(l, 0)
        g_drain(l, 1)
    out_ref[...] = bf(norm_rows(hidden, f32(gfin_ref[...])[None]))
    phase()


def solution(mesh):
    def device_fn(hidden_in, lengths, attn_norm, w_query, w_key, w_value, w_out, mlp_norm, w_gate, w_up, w_down, final_norm):
        batch, tok, d_model = hidden_in.shape
        layers, _, heads, head_dim = w_query.shape
        units = w_gate.shape[2]
        half = head_dim // 2
        freq = ROPE_BASE ** (-2.0 * np.arange(half, dtype=np.float32) / head_dim)
        freq = jnp.asarray(np.tile(freq.astype(np.float32), 4)[None])

        def by_rows(w):
            return jnp.transpose(w, (0, 2, 3, 1)).reshape(layers, heads * head_dim, d_model)

        part = heads // ROW
        wide = 2 * head_dim
        dma = pltpu.SemaphoreType.DMA
        b16 = jnp.bfloat16
        vm = pl.BlockSpec(memory_space=pltpu.VMEM)
        hbm = pl.BlockSpec(memory_space=pl.ANY)
        rtok = ROW * tok
        out = pl.pallas_call(
            kernel,
            name='prefill',
            out_shape=jax.ShapeDtypeStruct((tok, d_model), b16),
            in_specs=[vm, pl.BlockSpec(memory_space=pltpu.SMEM), vm, vm, vm, vm] + [hbm] * 7,
            out_specs=vm,
            scratch_shapes=[
                pltpu.VMEM((ROW, tok, d_model), b16),
                pltpu.VMEM((layers, part * head_dim, d_model), b16),
                pltpu.VMEM((layers, part, wide, d_model), b16),
                pltpu.VMEM((layers, heads * head_dim, d_model), b16),
                pltpu.VMEM((layers, ROW, 3, units, d_model), b16),
                pltpu.VMEM((part, rtok, wide), b16),
                pltpu.VMEM((COL, rtok, wide), b16),
                pltpu.VMEM((part, rtok, wide), b16),
                pltpu.VMEM((NY, rtok, wide), b16),
                pltpu.VMEM((NY * ROW, tok, wide), b16),
                pltpu.VMEM((NY * ROW, tok, wide), b16),
                pltpu.VMEM((2, tok, d_model), b16),
                pltpu.VMEM((COL, tok, d_model), b16),
                pltpu.VMEM((COL * tok, d_model), b16),
                pltpu.VMEM((2, ROW // 2 * COL * tok, ROW // 2 * units), b16),
                pltpu.VMEM((COL, tok, d_model), jnp.float32),
                pltpu.VMEM((COL - 1, tok, d_model), jnp.float32),
                dma((layers, 2 * part + 1)), dma((layers,)), dma((layers, 3)),
                dma((ROW - 1,)), dma((ROW - 1,)),
                dma((NZ, NY)), dma((NZ, NY)), dma((NY,)), dma((NY,)),
                dma((NY * ROW - 1,)), dma((NY * ROW - 1,)),
                dma((COL - 1,)), dma((COL - 1,)),
                dma((COL - 1,)), dma((COL - 1,)),
                dma((layers, 2, 9)), dma((layers, 2, 9)),
            ],
            compiler_params=pltpu.CompilerParams(collective_id=0, has_side_effects=True, vmem_limit_bytes=60 * 1024 * 1024),
        )(hidden_in.reshape(tok, d_model), lengths, attn_norm, mlp_norm, final_norm, freq,
          by_rows(w_query), by_rows(w_key), by_rows(w_value), w_out.reshape(layers, heads * head_dim, d_model),
          jnp.transpose(w_gate, (0, 2, 1)), jnp.transpose(w_up, (0, 2, 1)), w_down)
        return out.reshape(batch, tok, d_model)

    seq_part = P(None, 'tp', None)
    in_specs = (seq_part, P(), P(), P(), P(), P(), P(), P(), P(None, None, 'tp'), P(None, None, 'tp'), P(None, 'tp', None), P())
    return jax.shard_map(device_fn, mesh=mesh, in_specs=in_specs, out_specs=seq_part, check_vma=False)
```

```python
import functools

import jax
import jax.numpy as jnp
import numpy as np
from jax import lax
from jax.experimental import pallas as pl
from jax.experimental.pallas import tpu as pltpu
from jax.sharding import PartitionSpec as P

NORM_EPS = 1e-5
ROPE_BASE = 500000.0
MESH = pl.DeviceIdType.MESH
NX, NY, NZ = 4, 4, 4
ROW = 2 * NX
COL = NY * NZ

ROW_STEPS = [(2, 1), (2, 0), (1, 1), (3, 1), (1, 0), (3, 0), (0, 1)]
COL_STEPS = sorted(((dz, dy) for dz in range(NZ) for dy in range(NY) if dz or dy),
                   key=lambda s: min(s[0], 4 - s[0]) + min(s[1], 4 - s[1]))
PLANE_STEPS = sorted(((dy, dx, dc) for dy in range(NY) for dx in range(NX) for dc in range(2) if dy or dx or dc),
                     key=lambda s: -(min(s[0], 4 - s[0]) + min(s[1], 4 - s[1])))


class Phases:
    def __init__(self):
        self.open = None

    def __call__(self, name=None):
        if self.open is not None:
            self.open.__exit__(None, None, None)
        self.open = jax.named_scope(name) if name else None
        if name:
            self.open.__enter__()


def bf(v):
    return v.astype(jnp.bfloat16)


def f32(v):
    return v.astype(jnp.float32)


def dot_nt(a, b):
    return lax.dot_general(a, b, (((1,), (1,)), ((), ())), preferred_element_type=jnp.float32)


def norm_rows(h, gain):
    inv = lax.rsqrt(jnp.mean(h * h, axis=-1, keepdims=True) + NORM_EPS)
    return h * inv * gain


def kernel(h_in, len_in, gattn_in, gmlp_in, gfin_in, freq_in, wq_ref, wk_ref, wv_ref, wo_ref, wg_ref, wu_ref, wd_ref,
           out_ref,
           h_ref, len_ref, gattn_ref, gmlp_ref, gfin_ref, freq_ref, out_s, hrow, wq_s, wkv_s, wo_s, wm, kvs, kvbuf, qs, qbuf, cs, cbuf, hloc, hcol, zs, acts, ysend, ybuf,
           isem, lsem, wosem, msem, asend, arecv, kvsend, kvrecv, qsend, qrecv, csend, crecv, hsend, hrecv, ssend, srecv, gsend, grecv):
    phase = Phases()
    phase('start')
    layers = wo_s.shape[0]
    tok, d_model = h_ref.shape
    rtok = ROW * tok
    heads, wide = kvs.shape[0], kvs.shape[2]
    hd = wide // 2
    half = hd // 2
    units = wm.shape[3]
    me = lax.axis_index('tp')
    core = lax.rem(me, 2)
    i = lax.rem(me, ROW)
    x = i // 2
    r = me // ROW
    y = lax.rem(r, NY)
    z = r // NY

    def row_id(dx, dc):
        return 2 * lax.rem(x + (dx + NX) % NX, NX) + (1 - core if dc else core)

    def row_dev(dx, dc):
        return (r * ROW + row_id(dx, dc),)

    def y_at(dy):
        return lax.rem(y + (dy + NY) % NY, NY)

    def plane_dev(dy, dx, dc):
        return ((z * NY + y_at(dy)) * ROW + row_id(dx, dc),)

    def col_dev(dz, dy):
        return ((NY * lax.rem(z + (dz + NZ) % NZ, NZ) + y_at(dy)) * ROW + i,)

    def send(src, dst, ssem, rsem, dev):
        pltpu.make_async_remote_copy(src_ref=src, dst_ref=dst, send_sem=ssem, recv_sem=rsem, device_id=dev,
                                     device_id_type=MESH).start()

    def wait(ref, sem):
        pltpu.make_async_copy(ref, ref, sem).wait()

    def load(src, dst, sem):
        c = pltpu.make_async_copy(src, dst, sem)
        c.start()
        return c

    def load_qkv(l):
        base = i * (heads * hd)
        got = []
        for j in range(heads):
            rows = pl.ds(base + j * hd, hd)
            got.append(load(wk_ref.at[l, rows], wkv_s.at[l, j, 0:hd], lsem.at[l, 2 * j]))
            got.append(load(wv_ref.at[l, rows], wkv_s.at[l, j, hd:wide], lsem.at[l, 2 * j + 1]))
        got.append(load(wq_ref.at[l, pl.ds(base, heads * hd)], wq_s.at[l], lsem.at[l, 2 * heads]))
        return got

    def load_mlp(l):
        return [load(w.at[l], wm.at[l, i, k], msem.at[l, k]) for k, w in enumerate((wg_ref, wu_ref, wd_ref))]

    h_load = load(h_in, h_ref, isem.at[0])
    barrier = pltpu.get_barrier_semaphore()
    partners = [plane_dev(*s) for s in PLANE_STEPS] + [col_dev(*s) for s in COL_STEPS if s[0]]
    for dev in partners:
        pl.semaphore_signal(barrier, inc=1, device_id=dev, device_id_type=MESH)
    inputs = [load(src, dst, isem.at[k + 1]) for k, (src, dst) in enumerate((
        (freq_in, freq_ref), (gattn_in, gattn_ref), (gmlp_in, gmlp_ref), (gfin_in, gfin_ref),
        (len_in, len_ref)))]
    mlp_loads = [load_mlp(0)]
    qkv_loads = [load_qkv(0)]
    wo_loads = [load(wo_ref.at[0], wo_s.at[0], wosem.at[0])]
    mlp_loads.append(load_mlp(1))
    qkv_loads.append(load_qkv(1))
    wo_loads.append(load(wo_ref.at[1], wo_s.at[1], wosem.at[1]))
    for zz in range(1, NZ):
        @pl.when(zz > z)
        def _():
            kvbuf[zz * NY:(zz + 1) * NY] = jnp.zeros((NY, rtok, wide), kvbuf.dtype)
    phase('barrier')
    h_load.wait()
    pl.semaphore_wait(barrier, len(partners))

    hu = units // 2
    spans = (pl.ds(0, 2), pl.ds(2, 1))
    low, high = pl.ds(0, hu), pl.ds(hu, hu)

    def blk(l, p, dx, dc, rows=None):
        if rows is None:
            return wm.at[l, row_id(dx, dc), spans[p]]
        return wm.at[l, row_id(dx, dc), spans[p], rows]

    def g_push(l, p, k, ref, dx, dc):
        send(ref, ref, gsend.at[l, p, k], grecv.at[l, p, k], row_dev(dx, dc))

    def g_send(l, p):
        for c in (mlp_loads[l][:2], mlp_loads[l][2:])[p]:
            c.wait()
        own = blk(l, p, 0, 0)
        g_push(l, p, 1, own, 1, 0)
        g_push(l, p, 2, own, -1, 0)
        g_push(l, p, 0, own, 0, 1)

    def g_fwd(l, p):
        wait(blk(l, p, -1, 0), grecv.at[l, p, 1])
        g_push(l, p, 3, blk(l, p, -1, 0, low), 1, 0)
        wait(blk(l, p, 1, 0), grecv.at[l, p, 2])
        g_push(l, p, 4, blk(l, p, 1, 0, high), -1, 0)
        g_push(l, p, 5, blk(l, p, -1, 0), 0, 1)
        g_push(l, p, 6, blk(l, p, 1, 0), 0, 1)

    def g_fwd2(l, p):
        for k, rows in enumerate((low, high)):
            wait(blk(l, p, 2, 0, rows), grecv.at[l, p, 3 + k])
            g_push(l, p, 7 + k, blk(l, p, 2, 0, rows), 0, 1)

    def g_done(l, p):
        wait(blk(l, p, 0, 1), grecv.at[l, p, 0])
        wait(blk(l, p, -1, 1), grecv.at[l, p, 5])
        wait(blk(l, p, 1, 1), grecv.at[l, p, 6])
        for k, rows in enumerate((low, high)):
            wait(blk(l, p, 2, 1, rows), grecv.at[l, p, 7 + k])

    def g_drain(l, p):
        for k in (0, 1, 2, 5, 6):
            wait(blk(l, p, 0, 0), gsend.at[l, p, k])
        for k in (3, 4, 7, 8):
            wait(blk(l, p, 0, 0, low), gsend.at[l, p, k])


    def turned(p, c, s):
        swapped = jnp.where(lax.rem(lane, hd) < half, pltpu.roll(p, wide - half, 1), pltpu.roll(p, half, 1))
        return p * c + swapped * s

    for l in range(layers):
        phase(f'row_h#l={l}')
        if l == 0:
            for k, s in enumerate(ROW_STEPS):
                send(h_ref, hrow.at[i], asend.at[k], arecv.at[k], row_dev(*s))
            g_send(0, 0)
            hrow[pl.ds(i, 1)] = h_ref[...][None]
            for c in inputs:
                c.wait()
            lane = lax.broadcasted_iota(jnp.int32, (1, wide), 1)
            pos = f32(r * rtok + lax.broadcasted_iota(jnp.int32, (rtok, 1), 0))
            angles = pos * freq_ref[...]
            cos_tab = jnp.cos(angles)
            sin_tab = jnp.sin(angles)
            sin_tab = jnp.where(lax.rem(lane, hd) < half, -sin_tab, sin_tab)
        for k, (dx, dc) in enumerate(ROW_STEPS):
            wait(hrow.at[row_id(-dx, dc)], arecv.at[k])
        length = len_ref[0]
        if l == 1:
            g_fwd(1, 0)
        phase(f'qkv#l={l}')
        g_attn = f32(gattn_ref[...])[l:l + 1]
        g_mlp = f32(gmlp_ref[...])[l:l + 1]
        zs[0:rtok] = bf(norm_rows(f32(hrow[...]).reshape(rtok, d_model), g_attn))
        for c in qkv_loads[l]:
            c.wait()
        kv = dot_nt(zs[0:rtok], wkv_s[l].reshape(heads * wide, d_model))
        for j in range(heads):
            p = kv[:, j * wide:(j + 1) * wide]
            kvs[j] = bf(jnp.where(lane < hd, turned(p, cos_tab, sin_tab), p))
        for dz in (3, 2, 1, 0):
            @pl.when(z + dz < NZ)
            def _():
                for dy in (2, 1, 3, 0):
                    if dz or dy:
                        send(kvs.at[y_at(dy)], kvbuf.at[r], kvsend.at[dz, dy], kvrecv.at[dz, dy], col_dev(dz, dy))
        kvbuf[pl.ds(r, 1)] = kvs[pl.ds(y, 1)]
        q = dot_nt(zs[0:rtok], wq_s[l])
        for j in range(0, heads, 2):
            pair = turned(q[:, j * hd:(j + 2) * hd], cos_tab, sin_tab)
            qs[j] = bf(jnp.where(lane < hd, pair, 0.0))
            qs[j + 1] = bf(jnp.where(lane < hd, pltpu.roll(pair, hd, 1), 0.0))
        for dy in (2, 1, 3):
            send(qs.at[y_at(dy)], qbuf.at[y], qsend.at[dy], qrecv.at[dy], col_dev(0, dy))
        qbuf[pl.ds(y, 1)] = qs[pl.ds(y, 1)]
        phase(f'kv_wait#l={l}')
        for dy in (1, 3, 2):
            wait(qbuf.at[y_at(-dy)], qrecv.at[dy])
        for dz in range(NZ):
            @pl.when(z - dz >= 0)
            def _():
                for dy in range(NY):
                    if dz or dy:
                        wait(kvbuf.at[(z - dz) * NY + y_at(-dy)], kvrecv.at[dz, dy])
        for k in range(ROW - 1):
            wait(h_ref, asend.at[k])
        phase(f'attn#l={l}')
        keys = COL * rtok
        quer = NY * rtok
        kv_all = kvbuf[...].reshape(keys, wide)
        scores = dot_nt(qbuf[...].reshape(quer, wide), kv_all) * hd ** -0.5
        k_pos = lax.broadcasted_iota(jnp.int32, scores.shape, 1)
        q_pos = z * quer + lax.broadcasted_iota(jnp.int32, scores.shape, 0)
        scores = jnp.where((k_pos <= q_pos) & (k_pos < length), scores, -1e30)
        e = jnp.exp(scores - jnp.max(scores, axis=-1, keepdims=True))
        probs = bf(e * (1.0 / jnp.sum(e, axis=-1, keepdims=True)))
        pv = jnp.dot(probs, kv_all, preferred_element_type=jnp.float32)
        ctx = jnp.where(lax.rem(y, 2) == 0, pltpu.roll(pv, hd, 1), pv)
        cs[...] = bf(ctx.reshape(NY * ROW, tok, wide))
        phase(f'ctx#l={l}')
        slot = ROW * y + i
        for k, (dy, dx, dc) in enumerate(PLANE_STEPS):
            send(cs.at[ROW * y_at(dy) + row_id(dx, dc)], cbuf.at[slot], csend.at[k], crecv.at[k], plane_dev(dy, dx, dc))
        cbuf[pl.ds(slot, 1)] = cs[pl.ds(slot, 1)]
        phase(f'g_b#l={l}')
        if l == 0:
            g_send(0, 1)
            g_fwd(0, 0)
        else:
            g_fwd(1, 1)
        wo_loads[l].wait()
        phase(f'ctx_wait#l={l}')
        for k, (dy, dx, dc) in enumerate(PLANE_STEPS):
            wait(cbuf.at[ROW * y_at(-dy) + row_id(-dx, dc)], crecv.at[k])
        phase(f'out#l={l}')
        pieces = []
        for k in range(ROW):
            for j in range(0, heads, 2):
                pieces.append(jnp.where(lane < hd, cbuf[j * ROW + k], cbuf[(j + 1) * ROW + k]))
        ctx_all = jnp.concatenate(pieces, axis=1)
        for n in range(2):
            cols = slice(n * (d_model // 2), (n + 1) * (d_model // 2))
            attn_out = jnp.dot(ctx_all, wo_s[l, :, cols], preferred_element_type=jnp.float32)
            hid = bf(f32(h_ref[:, cols] if l == 0 else hloc[2 * l - 1, :, cols]) + attn_out)
            hloc[2 * l, :, cols] = hid
            hcol[0, :, cols] = hid
            for k, s in enumerate(COL_STEPS[:COL // 2 - 1]):
                send(hloc.at[2 * l, :, cols], hcol.at[k + 1, :, cols], hsend.at[k], hrecv.at[k], col_dev(*s))
        for k, s in list(enumerate(COL_STEPS))[COL // 2 - 1:]:
            send(hloc.at[2 * l], hcol.at[k + 1], hsend.at[k], hrecv.at[k], col_dev(*s))
        phase(f'col_h#l={l}')
        if l == 0:
            g_fwd(0, 1)
        g_fwd2(l, 0)
        grp = ROW // 2
        ulane = lax.broadcasted_iota(jnp.int32, (1, grp * units), 1) // units
        parts = 4
        width = d_model // parts
        halves = 1 if l == 0 else 2
        slots = COL // halves
        m = slots * tok
        for part in range(halves):
            phase(f'col_h_wait#l={l}#p={part}')
            for k in range(part * slots, (part + 1) * slots):
                if k:
                    wait(hcol.at[k], hrecv.at[k - 1])
            mine = slice(part * slots, (part + 1) * slots)
            zs[0:m] = bf(norm_rows(f32(hcol[mine]).reshape(m, d_model), g_mlp))
            if part == 0:
                phase(f'g_done#l={l}')
                g_done(l, 0)
            phase(f'mlp_up#l={l}#p={part}')
            for b in range(2):
                gate = dot_nt(zs[0:m], wm[l, b * grp:(b + 1) * grp, 0].reshape(grp * units, d_model))
                up = dot_nt(zs[0:m], wm[l, b * grp:(b + 1) * grp, 1].reshape(grp * units, d_model))
                act = bf(gate * (1.0 / (1.0 + jnp.exp(-gate))) * up)
                for j in range(grp):
                    acts[b, j * m:(j + 1) * m] = jnp.where(ulane == j, act, jnp.zeros_like(act))
                if part == 0 and b == 0:
                    phase(f'g_fwd2#l={l}')
                    g_fwd2(l, 1)
                    phase(f'mlp_up2#l={l}#p={part}')
            if part == 0:
                phase(f'g_done2#l={l}')
                if l == 0:
                    g_send(1, 0)
                g_done(l, 1)
            phase(f'mlp_down#l={l}#p={part}')
            for n in range(parts):
                cols = slice(n * width, (n + 1) * width)
                total = jnp.zeros((m, width), jnp.float32)
                for b in range(2):
                    wd = wm[l, b * grp:(b + 1) * grp, 2, :, cols].reshape(grp * units, width)
                    prod = jnp.dot(acts[b, 0:grp * m], wd, preferred_element_type=jnp.float32)
                    for j in range(grp):
                        total = total + f32(bf(prod[j * m:(j + 1) * m]))
                ysend[mine, :, cols] = total.reshape(slots, tok, width)
                for k in reversed(range(part * slots, (part + 1) * slots)):
                    if k:
                        dz, dy = COL_STEPS[k - 1]
                        send(ysend.at[k, :, cols], ybuf.at[k - 1, :, cols], ssend.at[k - 1], srecv.at[k - 1, n],
                             col_dev(-dz, -dy))
        phase(f'rs_wait#l={l}')
        for n in range(parts):
            cols = slice(n * width, (n + 1) * width)
            total = ysend[0, :, cols]
            for k in range(COL - 1):
                wait(ybuf.at[k, :, cols], srecv.at[k, n])
                total = total + ybuf[k, :, cols]
            hid = bf(f32(hloc[2 * l, :, cols]) + total)
            hloc[2 * l + 1, :, cols] = hid
            if l < layers - 1:
                hrow[pl.ds(i, 1), :, cols] = hid[None]
                for k, s in enumerate(ROW_STEPS):
                    send(hloc.at[2 * l + 1, :, cols], hrow.at[i, :, cols], asend.at[k], arecv.at[k], row_dev(*s))
        if l == 0:
            g_send(1, 1)
        phase(f'drain#l={l}')
        for k in range(len(PLANE_STEPS)):
            wait(cs.at[0], csend.at[k])
        for dz in range(NZ):
            @pl.when(z + dz < NZ)
            def _():
                for dy in range(NY):
                    if dz or dy:
                        wait(kvs.at[0], kvsend.at[dz, dy])
        for dy in (1, 2, 3):
            wait(qs.at[0], qsend.at[dy])
        for k in range(COL - 1):
            wait(hloc.at[2 * l], hsend.at[k])
            wait(ysend.at[0], ssend.at[k])
    phase('end')
    for l in range(layers):
        g_drain(l, 0)
        g_drain(l, 1)
    out_s[...] = bf(norm_rows(f32(hloc[2 * layers - 1]), f32(gfin_ref[...])[None]))
    c = load(out_s, out_ref, isem.at[0])
    c.wait()
    phase()


def solution(mesh):
    def device_fn(hidden_in, lengths, attn_norm, w_query, w_key, w_value, w_out, mlp_norm, w_gate, w_up, w_down, final_norm):
        batch, tok, d_model = hidden_in.shape
        layers, _, heads, head_dim = w_query.shape
        units = w_gate.shape[2]
        half = head_dim // 2
        freq = ROPE_BASE ** (-2.0 * np.arange(half, dtype=np.float32) / head_dim)
        freq = jnp.asarray(np.tile(freq.astype(np.float32), 4)[None])

        def by_rows(w):
            return jnp.transpose(w, (0, 2, 3, 1)).reshape(layers, heads * head_dim, d_model)

        part = heads // ROW
        wide = 2 * head_dim
        dma = pltpu.SemaphoreType.DMA
        b16 = jnp.bfloat16
        hbm = pl.BlockSpec(memory_space=pl.ANY)
        rtok = ROW * tok
        out = pl.pallas_call(
            kernel,
            name='prefill',
            out_shape=jax.ShapeDtypeStruct((tok, d_model), b16),
            in_specs=[hbm, pl.BlockSpec(memory_space=pltpu.HBM)] + [hbm] * 11,
            out_specs=hbm,
            scratch_shapes=[
                pltpu.VMEM((tok, d_model), b16),
                pltpu.SMEM((1,), jnp.int32),
                pltpu.VMEM((layers, d_model), b16),
                pltpu.VMEM((layers, d_model), b16),
                pltpu.VMEM((d_model,), b16),
                pltpu.VMEM((1, 4 * half), jnp.float32),
                pltpu.VMEM((tok, d_model), b16),
                pltpu.VMEM((ROW, tok, d_model), b16),
                pltpu.VMEM((layers, part * head_dim, d_model), b16),
                pltpu.VMEM((layers, part, wide, d_model), b16),
                pltpu.VMEM((layers, heads * head_dim, d_model), b16),
                pltpu.VMEM((layers, ROW, 3, units, d_model), b16),
                pltpu.VMEM((part, rtok, wide), b16),
                pltpu.VMEM((COL, rtok, wide), b16),
                pltpu.VMEM((part, rtok, wide), b16),
                pltpu.VMEM((NY, rtok, wide), b16),
                pltpu.VMEM((NY * ROW, tok, wide), b16),
                pltpu.VMEM((NY * ROW, tok, wide), b16),
                pltpu.VMEM((2 * layers, tok, d_model), b16),
                pltpu.VMEM((COL, tok, d_model), b16),
                pltpu.VMEM((COL * tok, d_model), b16),
                pltpu.VMEM((2, ROW // 2 * COL * tok, ROW // 2 * units), b16),
                pltpu.VMEM((COL, tok, d_model), jnp.float32),
                pltpu.VMEM((COL - 1, tok, d_model), jnp.float32),
                dma((6,)), dma((layers, 2 * part + 1)), dma((layers,)), dma((layers, 3)),
                dma((ROW - 1,)), dma((ROW - 1,)),
                dma((NZ, NY)), dma((NZ, NY)), dma((NY,)), dma((NY,)),
                dma((NY * ROW - 1,)), dma((NY * ROW - 1,)),
                dma((COL - 1,)), dma((COL - 1,)),
                dma((COL - 1,)), dma((COL - 1, 4)),
                dma((layers, 2, 9)), dma((layers, 2, 9)),
            ],
            compiler_params=pltpu.CompilerParams(collective_id=0, has_side_effects=True, vmem_limit_bytes=60 * 1024 * 1024),
        )(hidden_in.reshape(tok, d_model), lengths, attn_norm, mlp_norm, final_norm, freq,
          by_rows(w_query), by_rows(w_key), by_rows(w_value), w_out.reshape(layers, heads * head_dim, d_model),
          jnp.transpose(w_gate, (0, 2, 1)), jnp.transpose(w_up, (0, 2, 1)), w_down)
        return out.reshape(batch, tok, d_model)

    seq_part = P(None, 'tp', None)
    in_specs = (seq_part, P(), P(), P(), P(), P(), P(), P(), P(None, None, 'tp'), P(None, None, 'tp'), P(None, 'tp', None), P())
    return jax.shard_map(device_fn, mesh=mesh, in_specs=in_specs, out_specs=seq_part, check_vma=False)
```

```python
import functools

import jax
import jax.numpy as jnp
import numpy as np
from jax import lax
from jax.experimental import pallas as pl
from jax.experimental.pallas import tpu as pltpu
from jax.sharding import PartitionSpec as P

NORM_EPS = 1e-5
ROPE_BASE = 500000.0
MESH = pl.DeviceIdType.MESH
NX, NY, NZ = 4, 4, 4
ROW = 2 * NX
COL = NY * NZ

ROW_STEPS = [(2, 1), (2, 0), (1, 1), (3, 1), (1, 0), (3, 0), (0, 1)]
COL_STEPS = [(0, 2), (1, 0), (3, 0), (2, 0), (1, 2), (3, 2), (2, 2),
             (0, 1), (0, 3), (1, 1), (1, 3), (3, 1), (3, 3), (2, 1), (2, 3)]
SLOT = {s: k for k, s in enumerate([(0, 0)] + COL_STEPS)}
PLANE_STEPS = sorted(((dy, dx, dc) for dy in range(NY) for dx in range(NX) for dc in range(2) if dy or dx or dc),
                     key=lambda s: -(min(s[0], 4 - s[0]) + min(s[1], 4 - s[1])))


class Phases:
    def __init__(self):
        self.open = None

    def __call__(self, name=None):
        if self.open is not None:
            self.open.__exit__(None, None, None)
        self.open = jax.named_scope(name) if name else None
        if name:
            self.open.__enter__()


def bf(v):
    return v.astype(jnp.bfloat16)


def f32(v):
    return v.astype(jnp.float32)


def dot_nt(a, b):
    return lax.dot_general(a, b, (((1,), (1,)), ((), ())), preferred_element_type=jnp.float32)


def norm_rows(h, gain):
    inv = lax.rsqrt(jnp.mean(h * h, axis=-1, keepdims=True) + NORM_EPS)
    return h * inv * gain


def kernel(h_in, len_in, gattn_in, gmlp_in, gfin_in, freq_in, wq_ref, wk_ref, wv_ref, wo_ref, wg_ref, wu_ref, wd_ref,
           out_ref,
           h_ref, len_ref, gattn_ref, gmlp_ref, gfin_ref, freq_ref, hrow, wq_s, wkv_s, wo_s, wm, kvs, kvbuf, qs, qbuf, cs, cbuf, hloc, hcol, zs, acts, ysend, y1, yst, y2,
           isem, lsem, wosem, msem, asend, arecv, kvsend, kvrecv, qsend, qrecv, csend, crecv, hsend, hrecv, s1send, s1recv, s2send, s2recv, gsend, grecv):
    phase = Phases()
    phase('start')
    layers = wo_s.shape[0]
    tok, d_model = h_ref.shape
    rtok = ROW * tok
    heads, wide = kvs.shape[0], kvs.shape[2]
    hd = wide // 2
    half = hd // 2
    units = wm.shape[3]
    me = lax.axis_index('tp')
    core = lax.rem(me, 2)
    i = lax.rem(me, ROW)
    x = i // 2
    r = me // ROW
    y = lax.rem(r, NY)
    z = r // NY

    def row_id(dx, dc):
        return 2 * lax.rem(x + (dx + NX) % NX, NX) + (1 - core if dc else core)

    def row_dev(dx, dc):
        return (r * ROW + row_id(dx, dc),)

    def y_at(dy):
        return lax.rem(y + (dy + NY) % NY, NY)

    def plane_dev(dy, dx, dc):
        return ((z * NY + y_at(dy)) * ROW + row_id(dx, dc),)

    def col_dev(dz, dy):
        return ((NY * lax.rem(z + (dz + NZ) % NZ, NZ) + y_at(dy)) * ROW + i,)

    def first_slot(n, step, g):
        return SLOT[(g, step) if n % 2 == 0 else (step, g)]

    def back(n, step):
        return col_dev(0, -step) if n % 2 == 0 else col_dev(-step, 0)

    def send(src, dst, ssem, rsem, dev):
        pltpu.make_async_remote_copy(src_ref=src, dst_ref=dst, send_sem=ssem, recv_sem=rsem, device_id=dev,
                                     device_id_type=MESH).start()

    def wait(ref, sem):
        pltpu.make_async_copy(ref, ref, sem).wait()

    def load(src, dst, sem):
        c = pltpu.make_async_copy(src, dst, sem)
        c.start()
        return c

    def load_qkv(l):
        base = i * (heads * hd)
        got = []
        for j in range(heads):
            rows = pl.ds(base + j * hd, hd)
            got.append(load(wk_ref.at[l, rows], wkv_s.at[l, j, 0:hd], lsem.at[l, 2 * j]))
            got.append(load(wv_ref.at[l, rows], wkv_s.at[l, j, hd:wide], lsem.at[l, 2 * j + 1]))
        got.append(load(wq_ref.at[l, pl.ds(base, heads * hd)], wq_s.at[l], lsem.at[l, 2 * heads]))
        return got

    def load_mlp(l):
        return [load(w.at[l], wm.at[l, i, k], msem.at[l, k]) for k, w in enumerate((wg_ref, wu_ref, wd_ref))]

    h_load = load(h_in, h_ref, isem.at[0])
    barrier = pltpu.get_barrier_semaphore()
    partners = [plane_dev(*s) for s in PLANE_STEPS] + [col_dev(*s) for s in COL_STEPS if s[0]]
    for dev in partners:
        pl.semaphore_signal(barrier, inc=1, device_id=dev, device_id_type=MESH)
    inputs = [load(src, dst, isem.at[k + 1]) for k, (src, dst) in enumerate((
        (freq_in, freq_ref), (gattn_in, gattn_ref), (gmlp_in, gmlp_ref), (gfin_in, gfin_ref),
        (len_in, len_ref)))]
    mlp_loads = [load_mlp(0)]
    qkv_loads = [load_qkv(0)]
    wo_loads = [load(wo_ref.at[0], wo_s.at[0], wosem.at[0])]
    mlp_loads.append(load_mlp(1))
    qkv_loads.append(load_qkv(1))
    wo_loads.append(load(wo_ref.at[1], wo_s.at[1], wosem.at[1]))
    for zz in range(1, NZ):
        @pl.when(zz > z)
        def _():
            kvbuf[zz * NY:(zz + 1) * NY] = jnp.zeros((NY, rtok, wide), kvbuf.dtype)
    phase('barrier')
    h_load.wait()
    pl.semaphore_wait(barrier, len(partners))

    hu = units // 2
    spans = (pl.ds(0, 2), pl.ds(2, 1))
    low, high = pl.ds(0, hu), pl.ds(hu, hu)

    def blk(l, p, dx, dc, rows=None):
        if rows is None:
            return wm.at[l, row_id(dx, dc), spans[p]]
        return wm.at[l, row_id(dx, dc), spans[p], rows]

    def g_push(l, p, k, ref, dx, dc):
        send(ref, ref, gsend.at[l, p, k], grecv.at[l, p, k], row_dev(dx, dc))

    def g_send(l, p):
        for c in (mlp_loads[l][:2], mlp_loads[l][2:])[p]:
            c.wait()
        own = blk(l, p, 0, 0)
        g_push(l, p, 1, own, 1, 0)
        g_push(l, p, 2, own, -1, 0)
        g_push(l, p, 0, own, 0, 1)

    def g_fwd(l, p):
        wait(blk(l, p, -1, 0), grecv.at[l, p, 1])
        g_push(l, p, 3, blk(l, p, -1, 0, low), 1, 0)
        wait(blk(l, p, 1, 0), grecv.at[l, p, 2])
        g_push(l, p, 4, blk(l, p, 1, 0, high), -1, 0)
        g_push(l, p, 5, blk(l, p, -1, 0), 0, 1)
        g_push(l, p, 6, blk(l, p, 1, 0), 0, 1)

    def g_fwd2(l, p):
        for k, rows in enumerate((low, high)):
            wait(blk(l, p, 2, 0, rows), grecv.at[l, p, 3 + k])
            g_push(l, p, 7 + k, blk(l, p, 2, 0, rows), 0, 1)

    def g_done(l, p):
        wait(blk(l, p, 0, 1), grecv.at[l, p, 0])
        wait(blk(l, p, -1, 1), grecv.at[l, p, 5])
        wait(blk(l, p, 1, 1), grecv.at[l, p, 6])
        for k, rows in enumerate((low, high)):
            wait(blk(l, p, 2, 1, rows), grecv.at[l, p, 7 + k])

    def g_drain(l, p):
        for k in (0, 1, 2, 5, 6):
            wait(blk(l, p, 0, 0), gsend.at[l, p, k])
        for k in (3, 4, 7, 8):
            wait(blk(l, p, 0, 0, low), gsend.at[l, p, k])


    def turned(p, c, s):
        swapped = jnp.where(lax.rem(lane, hd) < half, pltpu.roll(p, wide - half, 1), pltpu.roll(p, half, 1))
        return p * c + swapped * s

    for l in range(layers):
        phase(f'row_h#l={l}')
        if l == 0:
            for k, s in enumerate(ROW_STEPS):
                send(h_ref, hrow.at[i], asend.at[k], arecv.at[k], row_dev(*s))
            g_send(0, 0)
            hrow[pl.ds(i, 1)] = h_ref[...][None]
            for c in inputs:
                c.wait()
            lane = lax.broadcasted_iota(jnp.int32, (1, wide), 1)
            pos = f32(r * rtok + lax.broadcasted_iota(jnp.int32, (rtok, 1), 0))
            angles = pos * freq_ref[...]
            cos_tab = jnp.cos(angles)
            sin_tab = jnp.sin(angles)
            sin_tab = jnp.where(lax.rem(lane, hd) < half, -sin_tab, sin_tab)
        for k, (dx, dc) in enumerate(ROW_STEPS):
            wait(hrow.at[row_id(-dx, dc)], arecv.at[k])
        length = len_ref[0]
        if l == 1:
            g_fwd(1, 0)
        phase(f'qkv#l={l}')
        g_attn = f32(gattn_ref[...])[l:l + 1]
        g_mlp = f32(gmlp_ref[...])[l:l + 1]
        zs[0:rtok] = bf(norm_rows(f32(hrow[...]).reshape(rtok, d_model), g_attn))
        for c in qkv_loads[l]:
            c.wait()
        kv = dot_nt(zs[0:rtok], wkv_s[l].reshape(heads * wide, d_model))
        for j in range(heads):
            p = kv[:, j * wide:(j + 1) * wide]
            kvs[j] = bf(jnp.where(lane < hd, turned(p, cos_tab, sin_tab), p))
        for dz in (3, 2, 1, 0):
            @pl.when(z + dz < NZ)
            def _():
                for dy in (2, 1, 3, 0):
                    if dz or dy:
                        send(kvs.at[y_at(dy)], kvbuf.at[r], kvsend.at[dz, dy], kvrecv.at[dz, dy], col_dev(dz, dy))
        kvbuf[pl.ds(r, 1)] = kvs[pl.ds(y, 1)]
        q = dot_nt(zs[0:rtok], wq_s[l])
        for j in range(0, heads, 2):
            pair = turned(q[:, j * hd:(j + 2) * hd], cos_tab, sin_tab)
            qs[j] = bf(jnp.where(lane < hd, pair, 0.0))
            qs[j + 1] = bf(jnp.where(lane < hd, pltpu.roll(pair, hd, 1), 0.0))
        for dy in (2, 1, 3):
            send(qs.at[y_at(dy)], qbuf.at[y], qsend.at[dy], qrecv.at[dy], col_dev(0, dy))
        qbuf[pl.ds(y, 1)] = qs[pl.ds(y, 1)]
        phase(f'kv_wait#l={l}')
        for dy in (1, 3, 2):
            wait(qbuf.at[y_at(-dy)], qrecv.at[dy])
        for dz in range(NZ):
            @pl.when(z - dz >= 0)
            def _():
                for dy in range(NY):
                    if dz or dy:
                        wait(kvbuf.at[(z - dz) * NY + y_at(-dy)], kvrecv.at[dz, dy])
        for k in range(ROW - 1):
            wait(h_ref, asend.at[k])
        phase(f'attn#l={l}')
        keys = COL * rtok
        quer = NY * rtok
        kv_all = kvbuf[...].reshape(keys, wide)
        scores = dot_nt(qbuf[...].reshape(quer, wide), kv_all) * hd ** -0.5
        k_pos = lax.broadcasted_iota(jnp.int32, scores.shape, 1)
        q_pos = z * quer + lax.broadcasted_iota(jnp.int32, scores.shape, 0)
        scores = jnp.where((k_pos <= q_pos) & (k_pos < length), scores, -1e30)
        e = jnp.exp(scores - jnp.max(scores, axis=-1, keepdims=True))
        probs = bf(e * (1.0 / jnp.sum(e, axis=-1, keepdims=True)))
        pv = jnp.dot(probs, kv_all, preferred_element_type=jnp.float32)
        ctx = jnp.where(lax.rem(y, 2) == 0, pltpu.roll(pv, hd, 1), pv)
        cs[...] = bf(ctx.reshape(NY * ROW, tok, wide))
        phase(f'ctx#l={l}')
        slot = ROW * y + i
        for k, (dy, dx, dc) in enumerate(PLANE_STEPS):
            send(cs.at[ROW * y_at(dy) + row_id(dx, dc)], cbuf.at[slot], csend.at[k], crecv.at[k], plane_dev(dy, dx, dc))
        cbuf[pl.ds(slot, 1)] = cs[pl.ds(slot, 1)]
        phase(f'g_b#l={l}')
        if l == 0:
            g_send(0, 1)
            g_fwd(0, 0)
        else:
            g_fwd(1, 1)
        wo_loads[l].wait()
        attn_out = jnp.zeros((tok, d_model), jnp.float32)
        for step in (0, 1, 3, 2):
            phase(f'ctx_wait#l={l}#s={step}')
            for k, (dy, dx, dc) in enumerate(PLANE_STEPS):
                if dx == step:
                    wait(cbuf.at[ROW * y_at(-dy) + row_id(-dx, dc)], crecv.at[k])
            phase(f'out#l={l}#s={step}')
            chip = lax.rem(x - step + NX, NX)
            pieces = []
            for c in range(2):
                for j in range(0, heads, 2):
                    pieces.append(jnp.where(lane < hd, cbuf[j * ROW + 2 * chip + c], cbuf[(j + 1) * ROW + 2 * chip + c]))
            ctx_chip = jnp.concatenate(pieces, axis=1)
            rows = pl.ds(pl.multiple_of(chip * (2 * heads * hd), 2 * heads * hd), 2 * heads * hd)
            if step != 2:
                attn_out = attn_out + jnp.dot(ctx_chip, wo_s[l, rows, :], preferred_element_type=jnp.float32)
        for n in range(2):
            cols = slice(n * (d_model // 2), (n + 1) * (d_model // 2))
            part_out = attn_out[:, cols] + jnp.dot(ctx_chip, wo_s[l, rows, cols], preferred_element_type=jnp.float32)
            hid = bf(f32(h_ref[:, cols] if l == 0 else hloc[2 * l - 1, :, cols]) + part_out)
            hloc[2 * l, :, cols] = hid
            hcol[0, :, cols] = hid
            for k, s in enumerate(COL_STEPS[:COL // 2 - 1]):
                send(hloc.at[2 * l, :, cols], hcol.at[k + 1, :, cols], hsend.at[k], hrecv.at[k], col_dev(*s))
        for k, s in list(enumerate(COL_STEPS))[COL // 2 - 1:]:
            send(hloc.at[2 * l], hcol.at[k + 1], hsend.at[k], hrecv.at[k], col_dev(*s))
        phase(f'col_h#l={l}')
        if l == 0:
            g_fwd(0, 1)
        g_fwd2(l, 0)
        if l == 1:
            g_fwd2(1, 1)
        grp = ROW // 2
        ulane = lax.broadcasted_iota(jnp.int32, (1, grp * units), 1) // units
        parts = 4
        width = d_model // parts
        halves = 1 if l == 0 else 2
        slots = COL // halves
        m = slots * tok
        for part in range(halves):
            phase(f'col_h_wait#l={l}#p={part}')
            for k in range(part * slots, (part + 1) * slots):
                if k:
                    wait(hcol.at[k], hrecv.at[k - 1])
            mine = slice(part * slots, (part + 1) * slots)
            zs[0:m] = bf(norm_rows(f32(hcol[mine]).reshape(m, d_model), g_mlp))
            if part == 0:
                phase(f'g_done#l={l}')
                g_done(l, 0)
            phase(f'mlp_up#l={l}#p={part}')
            for b in range(2):
                gate = dot_nt(zs[0:m], wm[l, b * grp:(b + 1) * grp, 0].reshape(grp * units, d_model))
                up = dot_nt(zs[0:m], wm[l, b * grp:(b + 1) * grp, 1].reshape(grp * units, d_model))
                act = bf(gate * (1.0 / (1.0 + jnp.exp(-gate))) * up)
                for j in range(grp):
                    acts[b, j * m:(j + 1) * m] = jnp.where(ulane == j, act, jnp.zeros_like(act))
                if l == 0 and b == 0:
                    phase(f'g_fwd2#l={l}')
                    g_fwd2(0, 1)
                    phase(f'mlp_up2#l={l}#p={part}')
            if part == 0:
                phase(f'g_done2#l={l}')
                if l == 0:
                    g_send(1, 0)
                g_done(l, 1)
            phase(f'mlp_down#l={l}#p={part}')
            for n in range(parts):
                cols = slice(n * width, (n + 1) * width)
                total = jnp.zeros((m, width), jnp.float32)
                for b in range(2):
                    wd = wm[l, b * grp:(b + 1) * grp, 2, :, cols].reshape(grp * units, width)
                    prod = jnp.dot(acts[b, 0:grp * m], wd, preferred_element_type=jnp.float32)
                    for j in range(grp):
                        total = total + f32(bf(prod[j * m:(j + 1) * m]))
                ysend[mine, :, cols] = total.reshape(slots, tok, width)
                for step in (2, 1, 3):
                    for g in range(4):
                        k = first_slot(n, step, g)
                        if part * slots <= k < (part + 1) * slots:
                            send(ysend.at[k, :, cols], y1.at[n, step - 1, g], s1send.at[n, step - 1], s1recv.at[n, step - 1],
                                 back(n, step))
        phase(f'rs_wait#l={l}')
        for n in range(parts):
            cols = slice(n * width, (n + 1) * width)
            sums = [ysend[first_slot(n, 0, g), :, cols] for g in range(4)]
            for step in (1, 3, 2):
                wait(y1.at[n, step - 1], s1recv.at[n, step - 1])
                sums = [t + y1[n, step - 1, g] for g, t in enumerate(sums)]
            for g in range(4):
                yst[n, g] = sums[g]
            for g in (2, 1, 3):
                send(yst.at[n, g], y2.at[n, g - 1], s2send.at[n, g - 1], s2recv.at[n, g - 1], back(n + 1, g))
        phase(f'rs2_wait#l={l}')
        for n in range(parts):
            cols = slice(n * width, (n + 1) * width)
            total = yst[n, 0]
            for g in (1, 3, 2):
                wait(y2.at[n, g - 1], s2recv.at[n, g - 1])
                total = total + y2[n, g - 1]
            hid = bf(f32(hloc[2 * l, :, cols]) + total)
            hloc[2 * l + 1, :, cols] = hid
            if l < layers - 1:
                hrow[pl.ds(i, 1), :, cols] = hid[None]
                for k, s in enumerate(ROW_STEPS):
                    send(hloc.at[2 * l + 1, :, cols], hrow.at[i, :, cols], asend.at[k], arecv.at[k], row_dev(*s))
        if l == 0:
            g_send(1, 1)
        phase(f'drain#l={l}')
        for k in range(len(PLANE_STEPS)):
            wait(cs.at[0], csend.at[k])
        for dz in range(NZ):
            @pl.when(z + dz < NZ)
            def _():
                for dy in range(NY):
                    if dz or dy:
                        wait(kvs.at[0], kvsend.at[dz, dy])
        for dy in (1, 2, 3):
            wait(qs.at[0], qsend.at[dy])
            for n in range(parts):
                wait(y1.at[n, dy - 1], s1send.at[n, dy - 1])
                wait(yst.at[n, dy], s2send.at[n, dy - 1])
        for k in range(COL - 1):
            wait(hloc.at[2 * l], hsend.at[k])
    phase('end')
    for l in range(layers):
        g_drain(l, 0)
        g_drain(l, 1)
    out_ref[...] = bf(norm_rows(f32(hloc[2 * layers - 1]), f32(gfin_ref[...])[None]))
    phase()


def solution(mesh):
    def device_fn(hidden_in, lengths, attn_norm, w_query, w_key, w_value, w_out, mlp_norm, w_gate, w_up, w_down, final_norm):
        batch, tok, d_model = hidden_in.shape
        layers, _, heads, head_dim = w_query.shape
        units = w_gate.shape[2]
        half = head_dim // 2
        freq = ROPE_BASE ** (-2.0 * np.arange(half, dtype=np.float32) / head_dim)
        freq = jnp.asarray(np.tile(freq.astype(np.float32), 4)[None])

        def by_rows(w):
            return jnp.transpose(w, (0, 2, 3, 1)).reshape(layers, heads * head_dim, d_model)

        part = heads // ROW
        wide = 2 * head_dim
        dma = pltpu.SemaphoreType.DMA
        b16 = jnp.bfloat16
        hbm = pl.BlockSpec(memory_space=pl.ANY)
        rtok = ROW * tok
        out = pl.pallas_call(
            kernel,
            name='prefill',
            out_shape=pltpu.VMEM((tok, d_model), b16),
            in_specs=[hbm, pl.BlockSpec(memory_space=pltpu.HBM)] + [hbm] * 11,
            out_specs=pl.BlockSpec(memory_space=pltpu.VMEM),
            scratch_shapes=[
                pltpu.VMEM((tok, d_model), b16),
                pltpu.SMEM((1,), jnp.int32),
                pltpu.VMEM((layers, d_model), b16),
                pltpu.VMEM((layers, d_model), b16),
                pltpu.VMEM((d_model,), b16),
                pltpu.VMEM((1, 4 * half), jnp.float32),
                pltpu.VMEM((ROW, tok, d_model), b16),
                pltpu.VMEM((layers, part * head_dim, d_model), b16),
                pltpu.VMEM((layers, part, wide, d_model), b16),
                pltpu.VMEM((layers, heads * head_dim, d_model), b16),
                pltpu.VMEM((layers, ROW, 3, units, d_model), b16),
                pltpu.VMEM((part, rtok, wide), b16),
                pltpu.VMEM((COL, rtok, wide), b16),
                pltpu.VMEM((part, rtok, wide), b16),
                pltpu.VMEM((NY, rtok, wide), b16),
                pltpu.VMEM((NY * ROW, tok, wide), b16),
                pltpu.VMEM((NY * ROW, tok, wide), b16),
                pltpu.VMEM((2 * layers, tok, d_model), b16),
                pltpu.VMEM((COL, tok, d_model), b16),
                pltpu.VMEM((COL * tok, d_model), b16),
                pltpu.VMEM((2, ROW // 2 * COL * tok, ROW // 2 * units), b16),
                pltpu.VMEM((COL, tok, d_model), jnp.float32),
                pltpu.VMEM((4, 3, 4, tok, d_model // 4), jnp.float32),
                pltpu.VMEM((4, 4, tok, d_model // 4), jnp.float32),
                pltpu.VMEM((4, 3, tok, d_model // 4), jnp.float32),
                dma((6,)), dma((layers, 2 * part + 1)), dma((layers,)), dma((layers, 3)),
                dma((ROW - 1,)), dma((ROW - 1,)),
                dma((NZ, NY)), dma((NZ, NY)), dma((NY,)), dma((NY,)),
                dma((NY * ROW - 1,)), dma((NY * ROW - 1,)),
                dma((COL - 1,)), dma((COL - 1,)),
                dma((4, 3)), dma((4, 3)), dma((4, 3)), dma((4, 3)),
                dma((layers, 2, 9)), dma((layers, 2, 9)),
            ],
            compiler_params=pltpu.CompilerParams(collective_id=0, has_side_effects=True, vmem_limit_bytes=60 * 1024 * 1024),
        )(hidden_in.reshape(tok, d_model), lengths, attn_norm, mlp_norm, final_norm, freq,
          by_rows(w_query), by_rows(w_key), by_rows(w_value), w_out.reshape(layers, heads * head_dim, d_model),
          jnp.transpose(w_gate, (0, 2, 1)), jnp.transpose(w_up, (0, 2, 1)), w_down)
        return out.reshape(batch, tok, d_model)

    seq_part = P(None, 'tp', None)
    in_specs = (seq_part, P(), P(), P(), P(), P(), P(), P(), P(None, None, 'tp'), P(None, None, 'tp'), P(None, 'tp', None), P())
    return jax.shard_map(device_fn, mesh=mesh, in_specs=in_specs, out_specs=seq_part, check_vma=False)
```

```python
import functools

import jax
import jax.numpy as jnp
import numpy as np
from jax import lax
from jax.experimental import pallas as pl
from jax.experimental.pallas import tpu as pltpu
from jax.sharding import PartitionSpec as P

NORM_EPS = 1e-5
ROPE_BASE = 500000.0
MESH = pl.DeviceIdType.MESH
NX, NY, NZ = 4, 4, 4
ROW = 2 * NX
COL = NY * NZ

ROW_STEPS = [(2, 1), (2, 0), (1, 1), (3, 1), (1, 0), (3, 0), (0, 1)]
COL_STEPS = [(0, 2), (1, 0), (3, 0), (2, 0), (1, 2), (3, 2), (2, 2),
             (0, 1), (0, 3), (1, 1), (1, 3), (3, 1), (3, 3), (2, 1), (2, 3)]
SLOT = {s: k for k, s in enumerate([(0, 0)] + COL_STEPS)}
PLANE_STEPS = sorted(((dy, dx, dc) for dy in range(NY) for dx in range(NX) for dc in range(2) if dy or dx or dc),
                     key=lambda s: -(min(s[0], 4 - s[0]) + min(s[1], 4 - s[1])))


class Phases:
    def __init__(self):
        self.open = None

    def __call__(self, name=None):
        if self.open is not None:
            self.open.__exit__(None, None, None)
        self.open = jax.named_scope(name) if name else None
        if name:
            self.open.__enter__()


def bf(v):
    return v.astype(jnp.bfloat16)


def f32(v):
    return v.astype(jnp.float32)


def dot_nt(a, b):
    return lax.dot_general(a, b, (((1,), (1,)), ((), ())), preferred_element_type=jnp.float32)


def norm_rows(h, gain):
    inv = lax.rsqrt(jnp.mean(h * h, axis=-1, keepdims=True) + NORM_EPS)
    return h * inv * gain


def kernel(h_in, len_in, gattn_in, gmlp_in, gfin_in, freq_in, wq_ref, wk_ref, wv_ref, wo_ref, wg_ref, wu_ref, wd_ref,
           out_ref,
           h_ref, len_ref, gattn_ref, gmlp_ref, gfin_ref, freq_ref, hrow, wq_s, wkv_s, wo_s, wm, kvs, kvbuf, qs, qbuf, cs, cbuf, hloc, hcol, zs, acts, ysend, y1, yst, y2,
           isem, lsem, wosem, msem, asend, arecv, kvsend, kvrecv, qsend, qrecv, csend, crecv, hsend, hrecv, s1send, s1recv, s2send, s2recv, gsend, grecv):
    phase = Phases()
    phase('start')
    layers = wo_s.shape[0]
    tok, d_model = h_ref.shape
    rtok = ROW * tok
    heads, wide = kvs.shape[0], kvs.shape[2]
    hd = wide // 2
    half = hd // 2
    units = wm.shape[3]
    me = lax.axis_index('tp')
    core = lax.rem(me, 2)
    i = lax.rem(me, ROW)
    x = i // 2
    r = me // ROW
    y = lax.rem(r, NY)
    z = r // NY

    def row_id(dx, dc):
        return 2 * lax.rem(x + (dx + NX) % NX, NX) + (1 - core if dc else core)

    def row_dev(dx, dc):
        return (r * ROW + row_id(dx, dc),)

    def y_at(dy):
        return lax.rem(y + (dy + NY) % NY, NY)

    def plane_dev(dy, dx, dc):
        return ((z * NY + y_at(dy)) * ROW + row_id(dx, dc),)

    def col_dev(dz, dy):
        return ((NY * lax.rem(z + (dz + NZ) % NZ, NZ) + y_at(dy)) * ROW + i,)

    def first_slot(n, step, g):
        return SLOT[(g, step) if n % 2 == 0 else (step, g)]

    def back(n, step):
        return col_dev(0, -step) if n % 2 == 0 else col_dev(-step, 0)

    def send(src, dst, ssem, rsem, dev):
        pltpu.make_async_remote_copy(src_ref=src, dst_ref=dst, send_sem=ssem, recv_sem=rsem, device_id=dev,
                                     device_id_type=MESH).start()

    def wait(ref, sem):
        pltpu.make_async_copy(ref, ref, sem).wait()

    def load(src, dst, sem):
        c = pltpu.make_async_copy(src, dst, sem)
        c.start()
        return c

    def load_qkv(l):
        base = i * (heads * hd)
        got = []
        for j in range(heads):
            rows = pl.ds(base + j * hd, hd)
            got.append(load(wk_ref.at[l, rows], wkv_s.at[l, j, 0:hd], lsem.at[l, 2 * j]))
            got.append(load(wv_ref.at[l, rows], wkv_s.at[l, j, hd:wide], lsem.at[l, 2 * j + 1]))
        got.append(load(wq_ref.at[l, pl.ds(base, heads * hd)], wq_s.at[l], lsem.at[l, 2 * heads]))
        return got

    def load_mlp(l):
        return [load(w.at[l], wm.at[l, i, k], msem.at[l, k]) for k, w in enumerate((wg_ref, wu_ref, wd_ref))]

    h_load = load(h_in, h_ref, isem.at[0])
    barrier = pltpu.get_barrier_semaphore()
    partners = [plane_dev(*s) for s in PLANE_STEPS] + [col_dev(*s) for s in COL_STEPS if s[0]]
    for dev in partners:
        pl.semaphore_signal(barrier, inc=1, device_id=dev, device_id_type=MESH)
    inputs = [load(src, dst, isem.at[k + 1]) for k, (src, dst) in enumerate((
        (freq_in, freq_ref), (gattn_in, gattn_ref), (gmlp_in, gmlp_ref), (gfin_in, gfin_ref),
        (len_in, len_ref)))]
    mlp_loads = [load_mlp(0)]
    qkv_loads = [load_qkv(0)]
    wo_loads = [load(wo_ref.at[0], wo_s.at[0], wosem.at[0])]
    mlp_loads.append(load_mlp(1))
    qkv_loads.append(load_qkv(1))
    wo_loads.append(load(wo_ref.at[1], wo_s.at[1], wosem.at[1]))
    for zz in range(1, NZ):
        @pl.when(zz > z)
        def _():
            kvbuf[zz * NY:(zz + 1) * NY] = jnp.zeros((NY, rtok, wide), kvbuf.dtype)
    phase('barrier')
    h_load.wait()
    pl.semaphore_wait(barrier, len(partners))

    hu = units // 2
    spans = (pl.ds(0, 2), pl.ds(2, 1))
    low, high = pl.ds(0, hu), pl.ds(hu, hu)

    def blk(l, p, dx, dc, rows=None):
        if rows is None:
            return wm.at[l, row_id(dx, dc), spans[p]]
        return wm.at[l, row_id(dx, dc), spans[p], rows]

    def g_push(l, p, k, ref, dx, dc):
        send(ref, ref, gsend.at[l, p, k], grecv.at[l, p, k], row_dev(dx, dc))

    def g_send(l, p):
        for c in (mlp_loads[l][:2], mlp_loads[l][2:])[p]:
            c.wait()
        own = blk(l, p, 0, 0)
        g_push(l, p, 1, own, 1, 0)
        g_push(l, p, 2, own, -1, 0)
        g_push(l, p, 0, own, 0, 1)

    def g_fwd(l, p):
        wait(blk(l, p, -1, 0), grecv.at[l, p, 1])
        g_push(l, p, 3, blk(l, p, -1, 0, low), 1, 0)
        wait(blk(l, p, 1, 0), grecv.at[l, p, 2])
        g_push(l, p, 4, blk(l, p, 1, 0, high), -1, 0)
        g_push(l, p, 5, blk(l, p, -1, 0), 0, 1)
        g_push(l, p, 6, blk(l, p, 1, 0), 0, 1)

    def g_fwd2(l, p):
        for k, rows in enumerate((low, high)):
            wait(blk(l, p, 2, 0, rows), grecv.at[l, p, 3 + k])
            g_push(l, p, 7 + k, blk(l, p, 2, 0, rows), 0, 1)

    def g_done(l, p):
        wait(blk(l, p, 0, 1), grecv.at[l, p, 0])
        wait(blk(l, p, -1, 1), grecv.at[l, p, 5])
        wait(blk(l, p, 1, 1), grecv.at[l, p, 6])
        for k, rows in enumerate((low, high)):
            wait(blk(l, p, 2, 1, rows), grecv.at[l, p, 7 + k])

    def g_drain(l, p):
        for k in (0, 1, 2, 5, 6):
            wait(blk(l, p, 0, 0), gsend.at[l, p, k])
        for k in (3, 4, 7, 8):
            wait(blk(l, p, 0, 0, low), gsend.at[l, p, k])


    def turned(p, c, s):
        swapped = jnp.where(lax.rem(lane, hd) < half, pltpu.roll(p, wide - half, 1), pltpu.roll(p, half, 1))
        return p * c + swapped * s

    for l in range(layers):
        phase(f'row_h#l={l}')
        if l == 0:
            for k, s in enumerate(ROW_STEPS):
                if s[1] == 0 or s[0] == 0:
                    send(h_ref, hrow.at[i], asend.at[k], arecv.at[k], row_dev(*s))
            g_send(0, 0)
            hrow[pl.ds(i, 1)] = h_ref[...][None]
            for c in inputs:
                c.wait()
            lane = lax.broadcasted_iota(jnp.int32, (1, wide), 1)
            pos = f32(r * rtok + lax.broadcasted_iota(jnp.int32, (rtok, 1), 0))
            angles = pos * freq_ref[...]
            cos_tab = jnp.cos(angles)
            sin_tab = jnp.sin(angles)
            sin_tab = jnp.where(lax.rem(lane, hd) < half, -sin_tab, sin_tab)
        if True:
            for dx in (1, 3, 2):
                wait(hrow.at[row_id(-dx, 0)], arecv.at[ROW_STEPS.index((dx, 0))])
                k = ROW_STEPS.index((dx, 1))
                send(hrow.at[row_id(-dx, 0)], hrow.at[row_id(-dx, 0)], asend.at[k], arecv.at[k], row_dev(0, 1))
        for k, (dx, dc) in enumerate(ROW_STEPS):
            if dc:
                wait(hrow.at[row_id(-dx, dc)], arecv.at[k])
        length = len_ref[0]
        if l == 1:
            g_fwd(1, 0)
        phase(f'qkv#l={l}')
        g_attn = f32(gattn_ref[...])[l:l + 1]
        g_mlp = f32(gmlp_ref[...])[l:l + 1]
        zs[0:rtok] = bf(norm_rows(f32(hrow[...]).reshape(rtok, d_model), g_attn))
        for c in qkv_loads[l]:
            c.wait()
        kv = dot_nt(zs[0:rtok], wkv_s[l].reshape(heads * wide, d_model))
        for j in range(heads):
            p = kv[:, j * wide:(j + 1) * wide]
            kvs[j] = bf(jnp.where(lane < hd, turned(p, cos_tab, sin_tab), p))
        for dz in (3, 2, 1, 0):
            @pl.when(z + dz < NZ)
            def _():
                for dy in (2, 1, 3, 0):
                    if dz or dy:
                        send(kvs.at[y_at(dy)], kvbuf.at[r], kvsend.at[dz, dy], kvrecv.at[dz, dy], col_dev(dz, dy))
        kvbuf[pl.ds(r, 1)] = kvs[pl.ds(y, 1)]
        q = dot_nt(zs[0:rtok], wq_s[l])
        for j in range(0, heads, 2):
            pair = turned(q[:, j * hd:(j + 2) * hd], cos_tab, sin_tab)
            qs[j] = bf(jnp.where(lane < hd, pair, 0.0))
            qs[j + 1] = bf(jnp.where(lane < hd, pltpu.roll(pair, hd, 1), 0.0))
        for dy in (2, 1, 3):
            send(qs.at[y_at(dy)], qbuf.at[y], qsend.at[dy], qrecv.at[dy], col_dev(0, dy))
        qbuf[pl.ds(y, 1)] = qs[pl.ds(y, 1)]
        phase(f'kv_wait#l={l}')
        for dy in (1, 3, 2):
            wait(qbuf.at[y_at(-dy)], qrecv.at[dy])
        for dz in range(NZ):
            @pl.when(z - dz >= 0)
            def _():
                for dy in range(NY):
                    if dz or dy:
                        wait(kvbuf.at[(z - dz) * NY + y_at(-dy)], kvrecv.at[dz, dy])
        for k in range(ROW - 1):
            wait(h_ref, asend.at[k])
        phase(f'attn#l={l}')
        keys = COL * rtok
        quer = NY * rtok
        kv_all = kvbuf[...].reshape(keys, wide)
        scores = dot_nt(qbuf[...].reshape(quer, wide), kv_all) * hd ** -0.5
        k_pos = lax.broadcasted_iota(jnp.int32, scores.shape, 1)
        q_pos = z * quer + lax.broadcasted_iota(jnp.int32, scores.shape, 0)
        scores = jnp.where((k_pos <= q_pos) & (k_pos < length), scores, -1e30)
        e = jnp.exp(scores - jnp.max(scores, axis=-1, keepdims=True))
        probs = bf(e * (1.0 / jnp.sum(e, axis=-1, keepdims=True)))
        pv = jnp.dot(probs, kv_all, preferred_element_type=jnp.float32)
        ctx = jnp.where(lax.rem(y, 2) == 0, pltpu.roll(pv, hd, 1), pv)
        cs[...] = bf(ctx.reshape(NY * ROW, tok, wide))
        phase(f'ctx#l={l}')
        slot = ROW * y + i
        for k, (dy, dx, dc) in enumerate(PLANE_STEPS):
            send(cs.at[ROW * y_at(dy) + row_id(dx, dc)], cbuf.at[slot], csend.at[k], crecv.at[k], plane_dev(dy, dx, dc))
        cbuf[pl.ds(slot, 1)] = cs[pl.ds(slot, 1)]
        phase(f'g_b#l={l}')
        if l == 0:
            g_send(0, 1)
            g_fwd(0, 0)
        else:
            g_fwd(1, 1)
        wo_loads[l].wait()
        attn_out = jnp.zeros((tok, d_model), jnp.float32)
        for step in (0, 1, 3, 2):
            phase(f'ctx_wait#l={l}#s={step}')
            for k, (dy, dx, dc) in enumerate(PLANE_STEPS):
                if dx == step:
                    wait(cbuf.at[ROW * y_at(-dy) + row_id(-dx, dc)], crecv.at[k])
            phase(f'out#l={l}#s={step}')
            chip = lax.rem(x - step + NX, NX)
            pieces = []
            for c in range(2):
                for j in range(0, heads, 2):
                    pieces.append(jnp.where(lane < hd, cbuf[j * ROW + 2 * chip + c], cbuf[(j + 1) * ROW + 2 * chip + c]))
            ctx_chip = jnp.concatenate(pieces, axis=1)
            rows = pl.ds(pl.multiple_of(chip * (2 * heads * hd), 2 * heads * hd), 2 * heads * hd)
            if step != 2:
                attn_out = attn_out + jnp.dot(ctx_chip, wo_s[l, rows, :], preferred_element_type=jnp.float32)
        for n in range(2):
            cols = slice(n * (d_model // 2), (n + 1) * (d_model // 2))
            part_out = attn_out[:, cols] + jnp.dot(ctx_chip, wo_s[l, rows, cols], preferred_element_type=jnp.float32)
            hid = bf(f32(h_ref[:, cols] if l == 0 else hloc[2 * l - 1, :, cols]) + part_out)
            hloc[2 * l, :, cols] = hid
            hcol[0, :, cols] = hid
            for k, s in enumerate(COL_STEPS[:COL // 2 - 1]):
                send(hloc.at[2 * l, :, cols], hcol.at[k + 1, :, cols], hsend.at[k], hrecv.at[k], col_dev(*s))
        for k, s in list(enumerate(COL_STEPS))[COL // 2 - 1:]:
            send(hloc.at[2 * l], hcol.at[k + 1], hsend.at[k], hrecv.at[k], col_dev(*s))
        phase(f'col_h#l={l}')
        if l == 0:
            g_fwd(0, 1)
        g_fwd2(l, 0)
        if l == 1:
            g_fwd2(1, 1)
        grp = ROW // 2
        ulane = lax.broadcasted_iota(jnp.int32, (1, grp * units), 1) // units
        parts = 4
        width = d_model // parts
        halves = 1 if l == 0 else 2
        slots = COL // halves
        m = slots * tok
        for part in range(halves):
            phase(f'col_h_wait#l={l}#p={part}')
            for k in range(part * slots, (part + 1) * slots):
                if k:
                    wait(hcol.at[k], hrecv.at[k - 1])
            mine = slice(part * slots, (part + 1) * slots)
            zs[0:m] = bf(norm_rows(f32(hcol[mine]).reshape(m, d_model), g_mlp))
            if part == 0:
                phase(f'g_done#l={l}')
                g_done(l, 0)
            phase(f'mlp_up#l={l}#p={part}')
            for b in range(2):
                gate = dot_nt(zs[0:m], wm[l, b * grp:(b + 1) * grp, 0].reshape(grp * units, d_model))
                up = dot_nt(zs[0:m], wm[l, b * grp:(b + 1) * grp, 1].reshape(grp * units, d_model))
                act = bf(gate * (1.0 / (1.0 + jnp.exp(-gate))) * up)
                for j in range(grp):
                    acts[b, j * m:(j + 1) * m] = jnp.where(ulane == j, act, jnp.zeros_like(act))
                if l == 0 and b == 0:
                    phase(f'g_fwd2#l={l}')
                    g_fwd2(0, 1)
                    phase(f'mlp_up2#l={l}#p={part}')
            if part == 0:
                phase(f'g_done2#l={l}')
                if l == 0:
                    g_send(1, 0)
                g_done(l, 1)
            phase(f'mlp_down#l={l}#p={part}')
            for n in range(parts):
                cols = slice(n * width, (n + 1) * width)
                total = jnp.zeros((m, width), jnp.float32)
                for b in range(2):
                    wd = wm[l, b * grp:(b + 1) * grp, 2, :, cols].reshape(grp * units, width)
                    prod = jnp.dot(acts[b, 0:grp * m], wd, preferred_element_type=jnp.float32)
                    for j in range(grp):
                        total = total + f32(bf(prod[j * m:(j + 1) * m]))
                ysend[mine, :, cols] = total.reshape(slots, tok, width)
                for step in (2, 1, 3):
                    for g in range(4):
                        k = first_slot(n, step, g)
                        if part * slots <= k < (part + 1) * slots:
                            send(ysend.at[k, :, cols], y1.at[n, step - 1, g], s1send.at[n, step - 1], s1recv.at[n, step - 1],
                                 back(n, step))
        phase(f'rs_wait#l={l}')
        for n in range(parts):
            cols = slice(n * width, (n + 1) * width)
            sums = [ysend[first_slot(n, 0, g), :, cols] for g in range(4)]
            for step in (1, 3, 2):
                wait(y1.at[n, step - 1], s1recv.at[n, step - 1])
                sums = [t + y1[n, step - 1, g] for g, t in enumerate(sums)]
            for g in range(4):
                yst[n, g] = sums[g]
            for g in (2, 1, 3):
                send(yst.at[n, g], y2.at[n, g - 1], s2send.at[n, g - 1], s2recv.at[n, g - 1], back(n + 1, g))
        phase(f'rs2_wait#l={l}')
        for n in range(parts):
            cols = slice(n * width, (n + 1) * width)
            total = yst[n, 0]
            for g in (1, 3, 2):
                wait(y2.at[n, g - 1], s2recv.at[n, g - 1])
                total = total + y2[n, g - 1]
            hid = bf(f32(hloc[2 * l, :, cols]) + total)
            hloc[2 * l + 1, :, cols] = hid
            if l < layers - 1:
                hrow[pl.ds(i, 1), :, cols] = hid[None]
                for k, s in enumerate(ROW_STEPS):
                    if s[1] == 0 or s[0] == 0:
                        send(hloc.at[2 * l + 1, :, cols], hrow.at[i, :, cols], asend.at[k], arecv.at[k], row_dev(*s))
        if l == 0:
            g_send(1, 1)
        phase(f'drain#l={l}')
        for k in range(len(PLANE_STEPS)):
            wait(cs.at[0], csend.at[k])
        for dz in range(NZ):
            @pl.when(z + dz < NZ)
            def _():
                for dy in range(NY):
                    if dz or dy:
                        wait(kvs.at[0], kvsend.at[dz, dy])
        for dy in (1, 2, 3):
            wait(qs.at[0], qsend.at[dy])
            for n in range(parts):
                wait(y1.at[n, dy - 1], s1send.at[n, dy - 1])
                wait(yst.at[n, dy], s2send.at[n, dy - 1])
        for k in range(COL - 1):
            wait(hloc.at[2 * l], hsend.at[k])
    phase('end')
    for l in range(layers):
        g_drain(l, 0)
        g_drain(l, 1)
    out_ref[...] = bf(norm_rows(f32(hloc[2 * layers - 1]), f32(gfin_ref[...])[None]))
    phase()


def solution(mesh):
    def device_fn(hidden_in, lengths, attn_norm, w_query, w_key, w_value, w_out, mlp_norm, w_gate, w_up, w_down, final_norm):
        batch, tok, d_model = hidden_in.shape
        layers, _, heads, head_dim = w_query.shape
        units = w_gate.shape[2]
        half = head_dim // 2
        freq = ROPE_BASE ** (-2.0 * np.arange(half, dtype=np.float32) / head_dim)
        freq = jnp.asarray(np.tile(freq.astype(np.float32), 4)[None])

        def by_rows(w):
            return jnp.transpose(w, (0, 2, 3, 1)).reshape(layers, heads * head_dim, d_model)

        part = heads // ROW
        wide = 2 * head_dim
        dma = pltpu.SemaphoreType.DMA
        b16 = jnp.bfloat16
        hbm = pl.BlockSpec(memory_space=pl.ANY)
        rtok = ROW * tok
        out = pl.pallas_call(
            kernel,
            name='prefill',
            out_shape=pltpu.VMEM((tok, d_model), b16),
            in_specs=[hbm, pl.BlockSpec(memory_space=pltpu.HBM)] + [hbm] * 11,
            out_specs=pl.BlockSpec(memory_space=pltpu.VMEM),
            scratch_shapes=[
                pltpu.VMEM((tok, d_model), b16),
                pltpu.SMEM((1,), jnp.int32),
                pltpu.VMEM((layers, d_model), b16),
                pltpu.VMEM((layers, d_model), b16),
                pltpu.VMEM((d_model,), b16),
                pltpu.VMEM((1, 4 * half), jnp.float32),
                pltpu.VMEM((ROW, tok, d_model), b16),
                pltpu.VMEM((layers, part * head_dim, d_model), b16),
                pltpu.VMEM((layers, part, wide, d_model), b16),
                pltpu.VMEM((layers, heads * head_dim, d_model), b16),
                pltpu.VMEM((layers, ROW, 3, units, d_model), b16),
                pltpu.VMEM((part, rtok, wide), b16),
                pltpu.VMEM((COL, rtok, wide), b16),
                pltpu.VMEM((part, rtok, wide), b16),
                pltpu.VMEM((NY, rtok, wide), b16),
                pltpu.VMEM((NY * ROW, tok, wide), b16),
                pltpu.VMEM((NY * ROW, tok, wide), b16),
                pltpu.VMEM((2 * layers, tok, d_model), b16),
                pltpu.VMEM((COL, tok, d_model), b16),
                pltpu.VMEM((COL * tok, d_model), b16),
                pltpu.VMEM((2, ROW // 2 * COL * tok, ROW // 2 * units), b16),
                pltpu.VMEM((COL, tok, d_model), jnp.float32),
                pltpu.VMEM((4, 3, 4, tok, d_model // 4), jnp.float32),
                pltpu.VMEM((4, 4, tok, d_model // 4), jnp.float32),
                pltpu.VMEM((4, 3, tok, d_model // 4), jnp.float32),
                dma((6,)), dma((layers, 2 * part + 1)), dma((layers,)), dma((layers, 3)),
                dma((ROW - 1,)), dma((ROW - 1,)),
                dma((NZ, NY)), dma((NZ, NY)), dma((NY,)), dma((NY,)),
                dma((NY * ROW - 1,)), dma((NY * ROW - 1,)),
                dma((COL - 1,)), dma((COL - 1,)),
                dma((4, 3)), dma((4, 3)), dma((4, 3)), dma((4, 3)),
                dma((layers, 2, 9)), dma((layers, 2, 9)),
            ],
            compiler_params=pltpu.CompilerParams(collective_id=0, has_side_effects=True, vmem_limit_bytes=60 * 1024 * 1024),
        )(hidden_in.reshape(tok, d_model), lengths, attn_norm, mlp_norm, final_norm, freq,
          by_rows(w_query), by_rows(w_key), by_rows(w_value), w_out.reshape(layers, heads * head_dim, d_model),
          jnp.transpose(w_gate, (0, 2, 1)), jnp.transpose(w_up, (0, 2, 1)), w_down)
        return out.reshape(batch, tok, d_model)

    seq_part = P(None, 'tp', None)
    in_specs = (seq_part, P(), P(), P(), P(), P(), P(), P(), P(None, None, 'tp'), P(None, None, 'tp'), P(None, 'tp', None), P())
    return jax.shard_map(device_fn, mesh=mesh, in_specs=in_specs, out_specs=seq_part, check_vma=False)
```

```python
import functools

import jax
import jax.numpy as jnp
import numpy as np
from jax import lax
from jax.experimental import pallas as pl
from jax.experimental.pallas import tpu as pltpu
from jax.sharding import PartitionSpec as P

NORM_EPS = 1e-5
ROPE_BASE = 500000.0
MESH = pl.DeviceIdType.MESH
NX, NY, NZ = 4, 4, 4
ROW = 2 * NX
COL = NY * NZ

ROW_STEPS = [(2, 1), (2, 0), (1, 1), (3, 1), (1, 0), (3, 0), (0, 1)]
COL_STEPS = [(0, 2), (1, 0), (3, 0), (2, 0), (1, 2), (3, 2), (2, 2),
             (0, 1), (0, 3), (1, 1), (1, 3), (3, 1), (3, 3), (2, 1), (2, 3)]
SLOT = {s: k for k, s in enumerate([(0, 0)] + COL_STEPS)}
PLANE_STEPS = sorted(((dy, dx, dc) for dy in range(NY) for dx in range(NX) for dc in range(2) if dy or dx or dc),
                     key=lambda s: -(min(s[0], 4 - s[0]) + min(s[1], 4 - s[1])))


class Phases:
    def __init__(self):
        self.open = None

    def __call__(self, name=None):
        if self.open is not None:
            self.open.__exit__(None, None, None)
        self.open = jax.named_scope(name) if name else None
        if name:
            self.open.__enter__()


def bf(v):
    return v.astype(jnp.bfloat16)


def f32(v):
    return v.astype(jnp.float32)


def dot_nt(a, b):
    return lax.dot_general(a, b, (((1,), (1,)), ((), ())), preferred_element_type=jnp.float32)


def norm_rows(h, gain):
    inv = lax.rsqrt(jnp.mean(h * h, axis=-1, keepdims=True) + NORM_EPS)
    return h * inv * gain


def kernel(h_in, len_in, gattn_in, gmlp_in, gfin_in, freq_in, wq_ref, wk_ref, wv_ref, wo_ref, wg_ref, wu_ref, wd_ref,
           out_ref,
           wkv_t, wq_t, wgu_t, h_ref, len_ref, gattn_ref, gmlp_ref, gfin_ref, freq_ref, hrow, wq_s, wkv_s, wo_s, wm, kvs, kvbuf, qs, qbuf, cs, cbuf, hloc, hcol, zs, acts, ysend, y1, yst, y2,
           isem, lsem, wosem, msem, asend, arecv, kvsend, kvrecv, qsend, qrecv, csend, crecv, hsend, hrecv, s1send, s1recv, s2send, s2recv, gsend, grecv):
    phase = Phases()
    phase('start')
    layers = wo_s.shape[0]
    tok, d_model = h_ref.shape
    rtok = ROW * tok
    heads, wide = kvs.shape[0], kvs.shape[2]
    hd = wide // 2
    half = hd // 2
    units = wm.shape[3]
    me = lax.axis_index('tp')
    core = lax.rem(me, 2)
    i = lax.rem(me, ROW)
    x = i // 2
    r = me // ROW
    y = lax.rem(r, NY)
    z = r // NY

    def row_id(dx, dc):
        return 2 * lax.rem(x + (dx + NX) % NX, NX) + (1 - core if dc else core)

    def row_dev(dx, dc):
        return (r * ROW + row_id(dx, dc),)

    def y_at(dy):
        return lax.rem(y + (dy + NY) % NY, NY)

    def plane_dev(dy, dx, dc):
        return ((z * NY + y_at(dy)) * ROW + row_id(dx, dc),)

    def col_dev(dz, dy):
        return ((NY * lax.rem(z + (dz + NZ) % NZ, NZ) + y_at(dy)) * ROW + i,)

    def first_slot(n, step, g):
        return SLOT[(g, step) if n % 2 == 0 else (step, g)]

    def back(n, step):
        return col_dev(0, -step) if n % 2 == 0 else col_dev(-step, 0)

    def send(src, dst, ssem, rsem, dev):
        pltpu.make_async_remote_copy(src_ref=src, dst_ref=dst, send_sem=ssem, recv_sem=rsem, device_id=dev,
                                     device_id_type=MESH).start()

    def wait(ref, sem):
        pltpu.make_async_copy(ref, ref, sem).wait()

    def load(src, dst, sem):
        c = pltpu.make_async_copy(src, dst, sem)
        c.start()
        return c

    def load_qkv(l):
        base = i * (heads * hd)
        got = []
        for j in range(heads):
            rows = pl.ds(base + j * hd, hd)
            got.append(load(wk_ref.at[l, rows], wkv_s.at[l, j, 0:hd], lsem.at[l, 2 * j]))
            got.append(load(wv_ref.at[l, rows], wkv_s.at[l, j, hd:wide], lsem.at[l, 2 * j + 1]))
        got.append(load(wq_ref.at[l, pl.ds(base, heads * hd)], wq_s.at[l], lsem.at[l, 2 * heads]))
        return got

    def load_mlp(l):
        return [load(w.at[l], wm.at[l, i, k], msem.at[l, k]) for k, w in enumerate((wg_ref, wu_ref, wd_ref))]

    h_load = load(h_in, h_ref, isem.at[0])
    barrier = pltpu.get_barrier_semaphore()
    partners = [plane_dev(*s) for s in PLANE_STEPS] + [col_dev(*s) for s in COL_STEPS if s[0]]
    for dev in partners:
        pl.semaphore_signal(barrier, inc=1, device_id=dev, device_id_type=MESH)
    inputs = [load(src, dst, isem.at[k + 1]) for k, (src, dst) in enumerate((
        (freq_in, freq_ref), (gattn_in, gattn_ref), (gmlp_in, gmlp_ref), (gfin_in, gfin_ref),
        (len_in, len_ref)))]
    mlp_loads = [load_mlp(0)]
    qkv_loads = [load_qkv(0)]
    wo_loads = [load(wo_ref.at[0], wo_s.at[0], wosem.at[0])]
    mlp_loads.append(load_mlp(1))
    qkv_loads.append(load_qkv(1))
    wo_loads.append(load(wo_ref.at[1], wo_s.at[1], wosem.at[1]))
    for zz in range(1, NZ):
        @pl.when(zz > z)
        def _():
            kvbuf[zz * NY:(zz + 1) * NY] = jnp.zeros((NY, rtok, wide), kvbuf.dtype)
    phase('barrier')
    h_load.wait()
    pl.semaphore_wait(barrier, len(partners))

    hu = units // 2
    spans = (pl.ds(0, 2), pl.ds(2, 1))
    low, high = pl.ds(0, hu), pl.ds(hu, hu)

    def blk(l, p, dx, dc, rows=None):
        if rows is None:
            return wm.at[l, row_id(dx, dc), spans[p]]
        return wm.at[l, row_id(dx, dc), spans[p], rows]

    def g_push(l, p, k, ref, dx, dc):
        send(ref, ref, gsend.at[l, p, k], grecv.at[l, p, k], row_dev(dx, dc))

    def g_send(l, p):
        for c in (mlp_loads[l][:2], mlp_loads[l][2:])[p]:
            c.wait()
        own = blk(l, p, 0, 0)
        g_push(l, p, 1, own, 1, 0)
        g_push(l, p, 2, own, -1, 0)
        g_push(l, p, 0, own, 0, 1)

    def g_fwd(l, p):
        wait(blk(l, p, -1, 0), grecv.at[l, p, 1])
        g_push(l, p, 3, blk(l, p, -1, 0, low), 1, 0)
        wait(blk(l, p, 1, 0), grecv.at[l, p, 2])
        g_push(l, p, 4, blk(l, p, 1, 0, high), -1, 0)
        g_push(l, p, 5, blk(l, p, -1, 0), 0, 1)
        g_push(l, p, 6, blk(l, p, 1, 0), 0, 1)

    def g_fwd2(l, p):
        for k, rows in enumerate((low, high)):
            wait(blk(l, p, 2, 0, rows), grecv.at[l, p, 3 + k])
            g_push(l, p, 7 + k, blk(l, p, 2, 0, rows), 0, 1)

    def g_done(l, p):
        wait(blk(l, p, 0, 1), grecv.at[l, p, 0])
        wait(blk(l, p, -1, 1), grecv.at[l, p, 5])
        wait(blk(l, p, 1, 1), grecv.at[l, p, 6])
        for k, rows in enumerate((low, high)):
            wait(blk(l, p, 2, 1, rows), grecv.at[l, p, 7 + k])

    def g_drain(l, p):
        for k in (0, 1, 2, 5, 6):
            wait(blk(l, p, 0, 0), gsend.at[l, p, k])
        for k in (3, 4, 7, 8):
            wait(blk(l, p, 0, 0, low), gsend.at[l, p, k])


    def turned(p, c, s):
        swapped = jnp.where(lax.rem(lane, hd) < half, pltpu.roll(p, wide - half, 1), pltpu.roll(p, half, 1))
        return p * c + swapped * s

    def turn_qkv(l):
        for c in qkv_loads[l]:
            c.wait()
        for j in range(heads):
            wkv_t[:, j * wide:(j + 1) * wide] = wkv_s[l, j].T
        for j in range(heads // 2):
            wq_t[:, j * wide:(j + 1) * wide] = wq_s[l, j * wide:(j + 1) * wide].T

    def turn_mlp(l):
        for j in range(0, ROW, 2):
            for k in range(2):
                wgu_t[k, :, j * units:(j + 2) * units] = wm[l, j:j + 2, k].reshape(2 * units, d_model).T

    for l in range(layers):
        phase(f'row_h#l={l}')
        if l == 0:
            for k, s in enumerate(ROW_STEPS):
                if s[1] == 0 or s[0] == 0:
                    send(h_ref, hrow.at[i], asend.at[k], arecv.at[k], row_dev(*s))
            g_send(0, 0)
            hrow[pl.ds(i, 1)] = h_ref[...][None]
            for c in inputs:
                c.wait()
            lane = lax.broadcasted_iota(jnp.int32, (1, wide), 1)
            pos = f32(r * rtok + lax.broadcasted_iota(jnp.int32, (rtok, 1), 0))
            angles = pos * freq_ref[...]
            cos_tab = jnp.cos(angles)
            sin_tab = jnp.sin(angles)
            sin_tab = jnp.where(lax.rem(lane, hd) < half, -sin_tab, sin_tab)
            phase('turn#l=0')
            turn_qkv(0)
            phase('row_wait#l=0')
        if True:
            for dx in (1, 3, 2):
                wait(hrow.at[row_id(-dx, 0)], arecv.at[ROW_STEPS.index((dx, 0))])
                k = ROW_STEPS.index((dx, 1))
                send(hrow.at[row_id(-dx, 0)], hrow.at[row_id(-dx, 0)], asend.at[k], arecv.at[k], row_dev(0, 1))
        for k, (dx, dc) in enumerate(ROW_STEPS):
            if dc:
                wait(hrow.at[row_id(-dx, dc)], arecv.at[k])
        length = len_ref[0]
        phase(f'qkv#l={l}')
        g_attn = f32(gattn_ref[...])[l:l + 1]
        g_mlp = f32(gmlp_ref[...])[l:l + 1]
        zs[0:rtok] = bf(norm_rows(f32(hrow[...]).reshape(rtok, d_model), g_attn))
        kv = jnp.dot(zs[0:rtok], wkv_t[...], preferred_element_type=jnp.float32)
        for j in range(heads):
            p = kv[:, j * wide:(j + 1) * wide]
            kvs[j] = bf(jnp.where(lane < hd, turned(p, cos_tab, sin_tab), p))
        for dz in (3, 2, 1, 0):
            @pl.when(z + dz < NZ)
            def _():
                for dy in (2, 1, 3, 0):
                    if dz or dy:
                        send(kvs.at[y_at(dy)], kvbuf.at[r], kvsend.at[dz, dy], kvrecv.at[dz, dy], col_dev(dz, dy))
        kvbuf[pl.ds(r, 1)] = kvs[pl.ds(y, 1)]
        q = jnp.dot(zs[0:rtok], wq_t[...], preferred_element_type=jnp.float32)
        for j in range(0, heads, 2):
            pair = turned(q[:, j * hd:(j + 2) * hd], cos_tab, sin_tab)
            qs[j] = bf(jnp.where(lane < hd, pair, 0.0))
            qs[j + 1] = bf(jnp.where(lane < hd, pltpu.roll(pair, hd, 1), 0.0))
        for dy in (2, 1, 3):
            send(qs.at[y_at(dy)], qbuf.at[y], qsend.at[dy], qrecv.at[dy], col_dev(0, dy))
        qbuf[pl.ds(y, 1)] = qs[pl.ds(y, 1)]
        phase(f'kv_wait#l={l}')
        for dy in (1, 3, 2):
            wait(qbuf.at[y_at(-dy)], qrecv.at[dy])
        for dz in range(NZ):
            @pl.when(z - dz >= 0)
            def _():
                for dy in range(NY):
                    if dz or dy:
                        wait(kvbuf.at[(z - dz) * NY + y_at(-dy)], kvrecv.at[dz, dy])
        for k in range(ROW - 1):
            wait(h_ref, asend.at[k])
        phase(f'attn#l={l}')
        keys = COL * rtok
        quer = NY * rtok
        kv_all = kvbuf[...].reshape(keys, wide)
        scores = dot_nt(qbuf[...].reshape(quer, wide), kv_all) * hd ** -0.5
        k_pos = lax.broadcasted_iota(jnp.int32, scores.shape, 1)
        q_pos = z * quer + lax.broadcasted_iota(jnp.int32, scores.shape, 0)
        scores = jnp.where((k_pos <= q_pos) & (k_pos < length), scores, -1e30)
        e = jnp.exp(scores - jnp.max(scores, axis=-1, keepdims=True))
        probs = bf(e * (1.0 / jnp.sum(e, axis=-1, keepdims=True)))
        pv = jnp.dot(probs, kv_all, preferred_element_type=jnp.float32)
        ctx = jnp.where(lax.rem(y, 2) == 0, pltpu.roll(pv, hd, 1), pv)
        cs[...] = bf(ctx.reshape(NY * ROW, tok, wide))
        phase(f'ctx#l={l}')
        slot = ROW * y + i
        for k, (dy, dx, dc) in enumerate(PLANE_STEPS):
            send(cs.at[ROW * y_at(dy) + row_id(dx, dc)], cbuf.at[slot], csend.at[k], crecv.at[k], plane_dev(dy, dx, dc))
        cbuf[pl.ds(slot, 1)] = cs[pl.ds(slot, 1)]
        phase(f'g_b#l={l}')
        if l == 0:
            g_send(0, 1)
            g_fwd(0, 0)
        else:
            g_fwd(1, 0)
            g_fwd(1, 1)
        wo_loads[l].wait()
        attn_out = jnp.zeros((tok, d_model), jnp.float32)
        for step in (0, 1, 3, 2):
            phase(f'ctx_wait#l={l}#s={step}')
            for k, (dy, dx, dc) in enumerate(PLANE_STEPS):
                if dx == step:
                    wait(cbuf.at[ROW * y_at(-dy) + row_id(-dx, dc)], crecv.at[k])
            phase(f'out#l={l}#s={step}')
            chip = lax.rem(x - step + NX, NX)
            pieces = []
            for c in range(2):
                for j in range(0, heads, 2):
                    pieces.append(jnp.where(lane < hd, cbuf[j * ROW + 2 * chip + c], cbuf[(j + 1) * ROW + 2 * chip + c]))
            ctx_chip = jnp.concatenate(pieces, axis=1)
            rows = pl.ds(pl.multiple_of(chip * (2 * heads * hd), 2 * heads * hd), 2 * heads * hd)
            if step != 2:
                attn_out = attn_out + jnp.dot(ctx_chip, wo_s[l, rows, :], preferred_element_type=jnp.float32)
        for n in range(2):
            cols = slice(n * (d_model // 2), (n + 1) * (d_model // 2))
            part_out = attn_out[:, cols] + jnp.dot(ctx_chip, wo_s[l, rows, cols], preferred_element_type=jnp.float32)
            hid = bf(f32(h_ref[:, cols] if l == 0 else hloc[2 * l - 1, :, cols]) + part_out)
            hloc[2 * l, :, cols] = hid
            hcol[0, :, cols] = hid
            for k, s in enumerate(COL_STEPS[:COL // 2 - 1]):
                send(hloc.at[2 * l, :, cols], hcol.at[k + 1, :, cols], hsend.at[k], hrecv.at[k], col_dev(*s))
        for k, s in list(enumerate(COL_STEPS))[COL // 2 - 1:]:
            send(hloc.at[2 * l], hcol.at[k + 1], hsend.at[k], hrecv.at[k], col_dev(*s))
        phase(f'col_h#l={l}')
        if l == 0:
            g_fwd(0, 1)
        g_fwd2(l, 0)
        if l == 1:
            g_done(1, 0)
            phase('turn_mlp')
            turn_mlp(1)
            phase(f'col_h2#l={l}')
            g_fwd2(1, 1)
        grp = ROW // 2
        ulane = lax.broadcasted_iota(jnp.int32, (1, grp * units), 1) // units
        parts = 4
        width = d_model // parts
        halves = 1 if l == 0 else 2
        slots = COL // halves
        m = slots * tok
        for part in range(halves):
            phase(f'col_h_wait#l={l}#p={part}')
            for k in range(part * slots, (part + 1) * slots):
                if k:
                    wait(hcol.at[k], hrecv.at[k - 1])
            mine = slice(part * slots, (part + 1) * slots)
            zs[0:m] = bf(norm_rows(f32(hcol[mine]).reshape(m, d_model), g_mlp))
            if l == 0:
                phase(f'g_done#l={l}')
                g_done(0, 0)
            phase(f'mlp_up#l={l}#p={part}')
            for b in range(2):
                if l == 0:
                    gate = dot_nt(zs[0:m], wm[l, b * grp:(b + 1) * grp, 0].reshape(grp * units, d_model))
                    up = dot_nt(zs[0:m], wm[l, b * grp:(b + 1) * grp, 1].reshape(grp * units, d_model))
                else:
                    these = slice(b * grp * units, (b + 1) * grp * units)
                    gate = jnp.dot(zs[0:m], wgu_t[0, :, these], preferred_element_type=jnp.float32)
                    up = jnp.dot(zs[0:m], wgu_t[1, :, these], preferred_element_type=jnp.float32)
                act = bf(gate * (1.0 / (1.0 + jnp.exp(-gate))) * up)
                for j in range(grp):
                    acts[b, j * m:(j + 1) * m] = jnp.where(ulane == j, act, jnp.zeros_like(act))
                if l == 0 and b == 0:
                    phase(f'g_fwd2#l={l}')
                    g_fwd2(0, 1)
                    phase(f'mlp_up2#l={l}#p={part}')
            if part == 0:
                phase(f'g_done2#l={l}')
                if l == 0:
                    g_send(1, 0)
                g_done(l, 1)
            phase(f'mlp_down#l={l}#p={part}')
            for n in range(parts):
                cols = slice(n * width, (n + 1) * width)
                total = jnp.zeros((m, width), jnp.float32)
                for b in range(2):
                    wd = wm[l, b * grp:(b + 1) * grp, 2, :, cols].reshape(grp * units, width)
                    prod = jnp.dot(acts[b, 0:grp * m], wd, preferred_element_type=jnp.float32)
                    for j in range(grp):
                        total = total + f32(bf(prod[j * m:(j + 1) * m]))
                ysend[mine, :, cols] = total.reshape(slots, tok, width)
                for step in (2, 1, 3):
                    for g in range(4):
                        k = first_slot(n, step, g)
                        if part * slots <= k < (part + 1) * slots:
                            send(ysend.at[k, :, cols], y1.at[n, step - 1, g], s1send.at[n, step - 1], s1recv.at[n, step - 1],
                                 back(n, step))
        if l == 0:
            phase('turn#l=1')
            turn_qkv(1)
        phase(f'rs_wait#l={l}')
        for n in range(parts):
            cols = slice(n * width, (n + 1) * width)
            sums = [ysend[first_slot(n, 0, g), :, cols] for g in range(4)]
            for step in (1, 3, 2):
                wait(y1.at[n, step - 1], s1recv.at[n, step - 1])
                sums = [t + y1[n, step - 1, g] for g, t in enumerate(sums)]
            for g in range(4):
                yst[n, g] = sums[g]
            for g in (2, 1, 3):
                send(yst.at[n, g], y2.at[n, g - 1], s2send.at[n, g - 1], s2recv.at[n, g - 1], back(n + 1, g))
        phase(f'rs2_wait#l={l}')
        for n in range(parts):
            cols = slice(n * width, (n + 1) * width)
            total = yst[n, 0]
            for g in (1, 3, 2):
                wait(y2.at[n, g - 1], s2recv.at[n, g - 1])
                total = total + y2[n, g - 1]
            hid = bf(f32(hloc[2 * l, :, cols]) + total)
            hloc[2 * l + 1, :, cols] = hid
            if l < layers - 1:
                hrow[pl.ds(i, 1), :, cols] = hid[None]
                for k, s in enumerate(ROW_STEPS):
                    if s[1] == 0 or s[0] == 0:
                        send(hloc.at[2 * l + 1, :, cols], hrow.at[i, :, cols], asend.at[k], arecv.at[k], row_dev(*s))
        if l == 0:
            g_send(1, 1)
        phase(f'drain#l={l}')
        for k in range(len(PLANE_STEPS)):
            wait(cs.at[0], csend.at[k])
        for dz in range(NZ):
            @pl.when(z + dz < NZ)
            def _():
                for dy in range(NY):
                    if dz or dy:
                        wait(kvs.at[0], kvsend.at[dz, dy])
        for dy in (1, 2, 3):
            wait(qs.at[0], qsend.at[dy])
            for n in range(parts):
                wait(y1.at[n, dy - 1], s1send.at[n, dy - 1])
                wait(yst.at[n, dy], s2send.at[n, dy - 1])
        for k in range(COL - 1):
            wait(hloc.at[2 * l], hsend.at[k])
    phase('end')
    for l in range(layers):
        g_drain(l, 0)
        g_drain(l, 1)
    out_ref[...] = bf(norm_rows(f32(hloc[2 * layers - 1]), f32(gfin_ref[...])[None]))
    phase()


def solution(mesh):
    def device_fn(hidden_in, lengths, attn_norm, w_query, w_key, w_value, w_out, mlp_norm, w_gate, w_up, w_down, final_norm):
        batch, tok, d_model = hidden_in.shape
        layers, _, heads, head_dim = w_query.shape
        units = w_gate.shape[2]
        half = head_dim // 2
        freq = ROPE_BASE ** (-2.0 * np.arange(half, dtype=np.float32) / head_dim)
        freq = jnp.asarray(np.tile(freq.astype(np.float32), 4)[None])

        def by_rows(w):
            return jnp.transpose(w, (0, 2, 3, 1)).reshape(layers, heads * head_dim, d_model)

        part = heads // ROW
        wide = 2 * head_dim
        dma = pltpu.SemaphoreType.DMA
        b16 = jnp.bfloat16
        hbm = pl.BlockSpec(memory_space=pl.ANY)
        rtok = ROW * tok
        out = pl.pallas_call(
            kernel,
            name='prefill',
            out_shape=pltpu.VMEM((tok, d_model), b16),
            in_specs=[hbm, pl.BlockSpec(memory_space=pltpu.HBM)] + [hbm] * 11,
            out_specs=pl.BlockSpec(memory_space=pltpu.VMEM),
            scratch_shapes=[
                pltpu.VMEM((d_model, part * wide), b16),
                pltpu.VMEM((d_model, part * head_dim), b16),
                pltpu.VMEM((2, d_model, ROW * units), b16),
                pltpu.VMEM((tok, d_model), b16),
                pltpu.SMEM((1,), jnp.int32),
                pltpu.VMEM((layers, d_model), b16),
                pltpu.VMEM((layers, d_model), b16),
                pltpu.VMEM((d_model,), b16),
                pltpu.VMEM((1, 4 * half), jnp.float32),
                pltpu.VMEM((ROW, tok, d_model), b16),
                pltpu.VMEM((layers, part * head_dim, d_model), b16),
                pltpu.VMEM((layers, part, wide, d_model), b16),
                pltpu.VMEM((layers, heads * head_dim, d_model), b16),
                pltpu.VMEM((layers, ROW, 3, units, d_model), b16),
                pltpu.VMEM((part, rtok, wide), b16),
                pltpu.VMEM((COL, rtok, wide), b16),
                pltpu.VMEM((part, rtok, wide), b16),
                pltpu.VMEM((NY, rtok, wide), b16),
                pltpu.VMEM((NY * ROW, tok, wide), b16),
                pltpu.VMEM((NY * ROW, tok, wide), b16),
                pltpu.VMEM((2 * layers, tok, d_model), b16),
                pltpu.VMEM((COL, tok, d_model), b16),
                pltpu.VMEM((COL * tok, d_model), b16),
                pltpu.VMEM((2, ROW // 2 * COL * tok, ROW // 2 * units), b16),
                pltpu.VMEM((COL, tok, d_model), jnp.float32),
                pltpu.VMEM((4, 3, 4, tok, d_model // 4), jnp.float32),
                pltpu.VMEM((4, 4, tok, d_model // 4), jnp.float32),
                pltpu.VMEM((4, 3, tok, d_model // 4), jnp.float32),
                dma((6,)), dma((layers, 2 * part + 1)), dma((layers,)), dma((layers, 3)),
                dma((ROW - 1,)), dma((ROW - 1,)),
                dma((NZ, NY)), dma((NZ, NY)), dma((NY,)), dma((NY,)),
                dma((NY * ROW - 1,)), dma((NY * ROW - 1,)),
                dma((COL - 1,)), dma((COL - 1,)),
                dma((4, 3)), dma((4, 3)), dma((4, 3)), dma((4, 3)),
                dma((layers, 2, 9)), dma((layers, 2, 9)),
            ],
            compiler_params=pltpu.CompilerParams(collective_id=0, has_side_effects=True, vmem_limit_bytes=60 * 1024 * 1024),
        )(hidden_in.reshape(tok, d_model), lengths, attn_norm, mlp_norm, final_norm, freq,
          by_rows(w_query), by_rows(w_key), by_rows(w_value), w_out.reshape(layers, heads * head_dim, d_model),
          jnp.transpose(w_gate, (0, 2, 1)), jnp.transpose(w_up, (0, 2, 1)), w_down)
        return out.reshape(batch, tok, d_model)

    seq_part = P(None, 'tp', None)
    in_specs = (seq_part, P(), P(), P(), P(), P(), P(), P(), P(None, None, 'tp'), P(None, None, 'tp'), P(None, 'tp', None), P())
    return jax.shard_map(device_fn, mesh=mesh, in_specs=in_specs, out_specs=seq_part, check_vma=False)
```

```python
import functools

import jax
import jax.numpy as jnp
import numpy as np
from jax import lax
from jax.experimental import pallas as pl
from jax.experimental.pallas import tpu as pltpu
from jax.sharding import PartitionSpec as P

NORM_EPS = 1e-5
ROPE_BASE = 500000.0
MESH = pl.DeviceIdType.MESH
NX, NY, NZ = 4, 4, 4
ROW = 2 * NX
COL = NY * NZ


def far(d):
    return min(d, NX - d)


ROW_STEPS = sorted(((dx, dc) for dx in range(NX) for dc in range(2) if dx or dc), key=lambda s: (-far(s[0]), -s[1]))
COL_STEPS = sorted(((dz, dy) for dz in range(NZ) for dy in range(NY) if dz or dy),
                   key=lambda s: (s[1] % 2, s[0] > 0, s[1] * (1 - s[1] % 2), far(s[0]), s))
SLOT = {s: k for k, s in enumerate([(0, 0)] + COL_STEPS)}
PLANE_STEPS = sorted(((dy, dx, dc) for dy in range(NY) for dx in range(NX) for dc in range(2) if dy or dx or dc),
                     key=lambda s: -far(s[0]) - far(s[1]))


class Phases:
    def __init__(self):
        self.open = None

    def __call__(self, name=None):
        if self.open is not None:
            self.open.__exit__(None, None, None)
        self.open = jax.named_scope(name) if name else None
        if name:
            self.open.__enter__()


def bf(v):
    return v.astype(jnp.bfloat16)


def f32(v):
    return v.astype(jnp.float32)


def dot_nt(a, b):
    return lax.dot_general(a, b, (((1,), (1,)), ((), ())), preferred_element_type=jnp.float32)


def norm_rows(h, gain):
    inv = lax.rsqrt(jnp.mean(h * h, axis=-1, keepdims=True) + NORM_EPS)
    return h * inv * gain


def kernel(h_in, len_in, gattn_in, gmlp_in, gfin_in, freq_in, wq_ref, wk_ref, wv_ref, wo_ref, wg_ref, wu_ref, wd_ref,
           out_ref,
           wkv_t, wq_t, wgu_t, h_ref, len_ref, gattn_ref, gmlp_ref, gfin_ref, freq_ref, hrow, wq_s, wkv_s, wo_s, wm, kvs, kvbuf, qs, qbuf, cs, cbuf, hloc, hcol, zs, acts, ysend, y1, yst, y2,
           isem, lsem, wosem, msem, asend, arecv, kvsend, kvrecv, qsend, qrecv, csend, crecv, hsend, hrecv, s1send, s1recv, s2send, s2recv, gsend, grecv):
    phase = Phases()
    phase('start')
    layers = wo_s.shape[0]
    tok, d_model = h_ref.shape
    rtok = ROW * tok
    heads, wide = kvs.shape[0], kvs.shape[2]
    hd = wide // 2
    half = hd // 2
    units = wm.shape[3]
    me = lax.axis_index('tp')
    core = lax.rem(me, 2)
    i = lax.rem(me, ROW)
    x = i // 2
    r = me // ROW
    y = lax.rem(r, NY)
    z = r // NY

    def row_id(dx, dc):
        return 2 * lax.rem(x + (dx + NX) % NX, NX) + (1 - core if dc else core)

    def row_dev(dx, dc):
        return (r * ROW + row_id(dx, dc),)

    def y_at(dy):
        return lax.rem(y + (dy + NY) % NY, NY)

    def plane_dev(dy, dx, dc):
        return ((z * NY + y_at(dy)) * ROW + row_id(dx, dc),)

    def col_dev(dz, dy):
        return ((NY * lax.rem(z + (dz + NZ) % NZ, NZ) + y_at(dy)) * ROW + i,)

    def first_slot(n, step, g):
        return SLOT[(g, step) if n % 2 == 0 else (step, g)]

    def back(n, step):
        return col_dev(0, -step) if n % 2 == 0 else col_dev(-step, 0)

    def send(src, dst, ssem, rsem, dev):
        pltpu.make_async_remote_copy(src_ref=src, dst_ref=dst, send_sem=ssem, recv_sem=rsem, device_id=dev,
                                     device_id_type=MESH).start()

    def wait(ref, sem):
        pltpu.make_async_copy(ref, ref, sem).wait()

    def load(src, dst, sem):
        c = pltpu.make_async_copy(src, dst, sem)
        c.start()
        return c

    def load_qkv(l):
        base = i * (heads * hd)
        got = []
        for j in range(heads):
            rows = pl.ds(base + j * hd, hd)
            got.append(load(wk_ref.at[l, rows], wkv_s.at[l, j, 0:hd], lsem.at[l, 2 * j]))
            got.append(load(wv_ref.at[l, rows], wkv_s.at[l, j, hd:wide], lsem.at[l, 2 * j + 1]))
        got.append(load(wq_ref.at[l, pl.ds(base, heads * hd)], wq_s.at[l], lsem.at[l, 2 * heads]))
        return got

    def load_mlp(l):
        return [load(w.at[l], wm.at[l, i, k], msem.at[l, k]) for k, w in enumerate((wg_ref, wu_ref, wd_ref))]

    h_load = load(h_in, h_ref, isem.at[0])
    barrier = pltpu.get_barrier_semaphore()
    partners = [plane_dev(*s) for s in PLANE_STEPS] + [col_dev(*s) for s in COL_STEPS if s[0]]
    for dev in partners:
        pl.semaphore_signal(barrier, inc=1, device_id=dev, device_id_type=MESH)
    inputs = [load(src, dst, isem.at[k + 1]) for k, (src, dst) in enumerate((
        (freq_in, freq_ref), (gattn_in, gattn_ref), (gmlp_in, gmlp_ref), (gfin_in, gfin_ref),
        (len_in, len_ref)))]
    mlp_loads = [load_mlp(0)]
    qkv_loads = [load_qkv(0)]
    wo_loads = [load(wo_ref.at[0], wo_s.at[0], wosem.at[0])]
    mlp_loads.append(load_mlp(1))
    qkv_loads.append(load_qkv(1))
    wo_loads.append(load(wo_ref.at[1], wo_s.at[1], wosem.at[1]))
    for zz in range(1, NZ):
        @pl.when(zz > z)
        def _():
            kvbuf[zz * NY:(zz + 1) * NY] = jnp.zeros((NY, rtok, wide), kvbuf.dtype)
    phase('barrier')
    h_load.wait()
    pl.semaphore_wait(barrier, len(partners))

    hu = units // 2
    spans = (pl.ds(0, 2), pl.ds(2, 1))
    low, high = pl.ds(0, hu), pl.ds(hu, hu)

    def blk(l, p, dx, dc, rows=None):
        if rows is None:
            return wm.at[l, row_id(dx, dc), spans[p]]
        return wm.at[l, row_id(dx, dc), spans[p], rows]

    def g_push(l, p, k, ref, dx, dc):
        send(ref, ref, gsend.at[l, p, k], grecv.at[l, p, k], row_dev(dx, dc))

    def g_send(l, p):
        for c in (mlp_loads[l][:2], mlp_loads[l][2:])[p]:
            c.wait()
        own = blk(l, p, 0, 0)
        g_push(l, p, 1, own, 1, 0)
        g_push(l, p, 2, own, -1, 0)
        g_push(l, p, 0, own, 0, 1)

    def g_fwd(l, p):
        wait(blk(l, p, -1, 0), grecv.at[l, p, 1])
        g_push(l, p, 3, blk(l, p, -1, 0, low), 1, 0)
        wait(blk(l, p, 1, 0), grecv.at[l, p, 2])
        g_push(l, p, 4, blk(l, p, 1, 0, high), -1, 0)
        g_push(l, p, 5, blk(l, p, -1, 0), 0, 1)
        g_push(l, p, 6, blk(l, p, 1, 0), 0, 1)

    def g_fwd2(l, p):
        for k, rows in enumerate((low, high)):
            wait(blk(l, p, 2, 0, rows), grecv.at[l, p, 3 + k])
            g_push(l, p, 7 + k, blk(l, p, 2, 0, rows), 0, 1)

    def g_done(l, p):
        wait(blk(l, p, 0, 1), grecv.at[l, p, 0])
        wait(blk(l, p, -1, 1), grecv.at[l, p, 5])
        wait(blk(l, p, 1, 1), grecv.at[l, p, 6])
        for k, rows in enumerate((low, high)):
            wait(blk(l, p, 2, 1, rows), grecv.at[l, p, 7 + k])

    def g_drain(l, p):
        for k in (0, 1, 2, 5, 6):
            wait(blk(l, p, 0, 0), gsend.at[l, p, k])
        for k in (3, 4, 7, 8):
            wait(blk(l, p, 0, 0, low), gsend.at[l, p, k])


    def turned(p, c, s):
        swapped = jnp.where(lax.rem(lane, hd) < half, pltpu.roll(p, wide - half, 1), pltpu.roll(p, half, 1))
        return p * c + swapped * s

    def turn_qkv(l):
        for c in qkv_loads[l]:
            c.wait()
        for j in range(heads):
            wkv_t[:, j * wide:(j + 1) * wide] = wkv_s[l, j].T
        for j in range(heads // 2):
            wq_t[:, j * wide:(j + 1) * wide] = wq_s[l, j * wide:(j + 1) * wide].T

    def turn_mlp(l):
        for j in range(0, ROW, 2):
            for k in range(2):
                wgu_t[k, :, j * units:(j + 2) * units] = wm[l, j:j + 2, k].reshape(2 * units, d_model).T

    for l in range(layers):
        phase(f'row_h#l={l}')
        if l == 0:
            for k, s in enumerate(ROW_STEPS):
                if s[1] == 0 or s[0] == 0:
                    send(h_ref, hrow.at[i], asend.at[k], arecv.at[k], row_dev(*s))
            g_send(0, 0)
            hrow[pl.ds(i, 1)] = h_ref[...][None]
            for c in inputs:
                c.wait()
            lane = lax.broadcasted_iota(jnp.int32, (1, wide), 1)
            pos = f32(r * rtok + lax.broadcasted_iota(jnp.int32, (rtok, 1), 0))
            angles = pos * freq_ref[...]
            cos_tab = jnp.cos(angles)
            sin_tab = jnp.sin(angles)
            sin_tab = jnp.where(lax.rem(lane, hd) < half, -sin_tab, sin_tab)
            phase('turn#l=0')
            turn_qkv(0)
            phase('row_wait#l=0')
        if True:
            for dx in (1, 3, 2):
                wait(hrow.at[row_id(-dx, 0)], arecv.at[ROW_STEPS.index((dx, 0))])
                k = ROW_STEPS.index((dx, 1))
                send(hrow.at[row_id(-dx, 0)], hrow.at[row_id(-dx, 0)], asend.at[k], arecv.at[k], row_dev(0, 1))
        for k, (dx, dc) in enumerate(ROW_STEPS):
            if dc:
                wait(hrow.at[row_id(-dx, dc)], arecv.at[k])
        length = len_ref[0]
        phase(f'qkv#l={l}')
        g_attn = f32(gattn_ref[...])[l:l + 1]
        g_mlp = f32(gmlp_ref[...])[l:l + 1]
        zs[0:rtok] = bf(norm_rows(f32(hrow[...]).reshape(rtok, d_model), g_attn))
        kv = jnp.dot(zs[0:rtok], wkv_t[...], preferred_element_type=jnp.float32)
        for j in range(heads):
            p = kv[:, j * wide:(j + 1) * wide]
            kvs[j] = bf(jnp.where(lane < hd, turned(p, cos_tab, sin_tab), p))
        for dz in (3, 2, 1, 0):
            @pl.when(z + dz < NZ)
            def _():
                for dy in (2, 1, 3, 0):
                    if dz or dy:
                        send(kvs.at[y_at(dy)], kvbuf.at[r], kvsend.at[dz, dy], kvrecv.at[dz, dy], col_dev(dz, dy))
        kvbuf[pl.ds(r, 1)] = kvs[pl.ds(y, 1)]
        q = jnp.dot(zs[0:rtok], wq_t[...], preferred_element_type=jnp.float32)
        for j in range(0, heads, 2):
            pair = turned(q[:, j * hd:(j + 2) * hd], cos_tab, sin_tab)
            qs[j] = bf(jnp.where(lane < hd, pair, 0.0))
            qs[j + 1] = bf(jnp.where(lane < hd, pltpu.roll(pair, hd, 1), 0.0))
        for dy in (2, 1, 3):
            send(qs.at[y_at(dy)], qbuf.at[y], qsend.at[dy], qrecv.at[dy], col_dev(0, dy))
        qbuf[pl.ds(y, 1)] = qs[pl.ds(y, 1)]
        phase(f'kv_wait#l={l}')
        for dy in (1, 3, 2):
            wait(qbuf.at[y_at(-dy)], qrecv.at[dy])
        for dz in range(NZ):
            @pl.when(z - dz >= 0)
            def _():
                for dy in range(NY):
                    if dz or dy:
                        wait(kvbuf.at[(z - dz) * NY + y_at(-dy)], kvrecv.at[dz, dy])
        for k in range(ROW - 1):
            wait(h_ref, asend.at[k])
        phase(f'attn#l={l}')
        keys = COL * rtok
        quer = NY * rtok
        kv_all = kvbuf[...].reshape(keys, wide)
        scores = dot_nt(qbuf[...].reshape(quer, wide), kv_all) * hd ** -0.5
        k_pos = lax.broadcasted_iota(jnp.int32, scores.shape, 1)
        q_pos = z * quer + lax.broadcasted_iota(jnp.int32, scores.shape, 0)
        scores = jnp.where((k_pos <= q_pos) & (k_pos < length), scores, -1e30)
        e = jnp.exp(scores - jnp.max(scores, axis=-1, keepdims=True))
        probs = bf(e * (1.0 / jnp.sum(e, axis=-1, keepdims=True)))
        pv = jnp.dot(probs, kv_all, preferred_element_type=jnp.float32)
        ctx = jnp.where(lax.rem(y, 2) == 0, pltpu.roll(pv, hd, 1), pv)
        cs[...] = bf(ctx.reshape(NY * ROW, tok, wide))
        phase(f'ctx#l={l}')
        slot = ROW * y + i
        for k, (dy, dx, dc) in enumerate(PLANE_STEPS):
            send(cs.at[ROW * y_at(dy) + row_id(dx, dc)], cbuf.at[slot], csend.at[k], crecv.at[k], plane_dev(dy, dx, dc))
        cbuf[pl.ds(slot, 1)] = cs[pl.ds(slot, 1)]
        phase(f'g_b#l={l}')
        if l == 0:
            g_send(0, 1)
            g_fwd(0, 0)
        else:
            g_fwd(1, 0)
            g_fwd(1, 1)
        wo_loads[l].wait()
        attn_out = jnp.zeros((tok, d_model), jnp.float32)
        for step in (0, 1, 3, 2):
            phase(f'ctx_wait#l={l}#s={step}')
            for k, (dy, dx, dc) in enumerate(PLANE_STEPS):
                if dx == step:
                    wait(cbuf.at[ROW * y_at(-dy) + row_id(-dx, dc)], crecv.at[k])
            phase(f'out#l={l}#s={step}')
            chip = lax.rem(x - step + NX, NX)
            pieces = []
            for c in range(2):
                for j in range(0, heads, 2):
                    pieces.append(jnp.where(lane < hd, cbuf[j * ROW + 2 * chip + c], cbuf[(j + 1) * ROW + 2 * chip + c]))
            ctx_chip = jnp.concatenate(pieces, axis=1)
            rows = pl.ds(pl.multiple_of(chip * (2 * heads * hd), 2 * heads * hd), 2 * heads * hd)
            if step != 2:
                attn_out = attn_out + jnp.dot(ctx_chip, wo_s[l, rows, :], preferred_element_type=jnp.float32)
        for n in range(2):
            cols = slice(n * (d_model // 2), (n + 1) * (d_model // 2))
            part_out = attn_out[:, cols] + jnp.dot(ctx_chip, wo_s[l, rows, cols], preferred_element_type=jnp.float32)
            hid = bf(f32(h_ref[:, cols] if l == 0 else hloc[2 * l - 1, :, cols]) + part_out)
            hloc[2 * l, :, cols] = hid
            hcol[0, :, cols] = hid
            for k, s in enumerate(COL_STEPS[:COL // 2 - 1]):
                send(hloc.at[2 * l, :, cols], hcol.at[k + 1, :, cols], hsend.at[k], hrecv.at[k], col_dev(*s))
        for k, s in list(enumerate(COL_STEPS))[COL // 2 - 1:]:
            send(hloc.at[2 * l], hcol.at[k + 1], hsend.at[k], hrecv.at[k], col_dev(*s))
        phase(f'col_h#l={l}')
        if l == 0:
            g_fwd(0, 1)
        g_fwd2(l, 0)
        if l == 1:
            g_done(1, 0)
            phase('turn_mlp')
            turn_mlp(1)
            phase(f'col_h2#l={l}')
            g_fwd2(1, 1)
        grp = ROW // 2
        ulane = lax.broadcasted_iota(jnp.int32, (1, grp * units), 1) // units
        parts = 4
        width = d_model // parts
        halves = 1 if l == 0 else 2
        slots = COL // halves
        m = slots * tok
        for part in range(halves):
            phase(f'col_h_wait#l={l}#p={part}')
            for k in range(part * slots, (part + 1) * slots):
                if k:
                    wait(hcol.at[k], hrecv.at[k - 1])
            mine = slice(part * slots, (part + 1) * slots)
            zs[0:m] = bf(norm_rows(f32(hcol[mine]).reshape(m, d_model), g_mlp))
            if l == 0:
                phase(f'g_done#l={l}')
                g_done(0, 0)
            phase(f'mlp_up#l={l}#p={part}')
            for b in range(2):
                if l == 0:
                    gate = dot_nt(zs[0:m], wm[l, b * grp:(b + 1) * grp, 0].reshape(grp * units, d_model))
                    up = dot_nt(zs[0:m], wm[l, b * grp:(b + 1) * grp, 1].reshape(grp * units, d_model))
                else:
                    these = slice(b * grp * units, (b + 1) * grp * units)
                    gate = jnp.dot(zs[0:m], wgu_t[0, :, these], preferred_element_type=jnp.float32)
                    up = jnp.dot(zs[0:m], wgu_t[1, :, these], preferred_element_type=jnp.float32)
                act = bf(gate * (1.0 / (1.0 + jnp.exp(-gate))) * up)
                for j in range(grp):
                    acts[b, j * m:(j + 1) * m] = jnp.where(ulane == j, act, jnp.zeros_like(act))
                if l == 0 and b == 0:
                    phase(f'g_fwd2#l={l}')
                    g_fwd2(0, 1)
                    phase(f'mlp_up2#l={l}#p={part}')
            if part == 0:
                phase(f'g_done2#l={l}')
                if l == 0:
                    g_send(1, 0)
                g_done(l, 1)
            phase(f'mlp_down#l={l}#p={part}')
            for n in range(parts):
                cols = slice(n * width, (n + 1) * width)
                total = jnp.zeros((m, width), jnp.float32)
                for b in range(2):
                    wd = wm[l, b * grp:(b + 1) * grp, 2, :, cols].reshape(grp * units, width)
                    prod = jnp.dot(acts[b, 0:grp * m], wd, preferred_element_type=jnp.float32)
                    for j in range(grp):
                        total = total + f32(bf(prod[j * m:(j + 1) * m]))
                ysend[mine, :, cols] = total.reshape(slots, tok, width)
                for step in (2, 1, 3):
                    for g in range(4):
                        k = first_slot(n, step, g)
                        if part * slots <= k < (part + 1) * slots:
                            send(ysend.at[k, :, cols], y1.at[n, step - 1, g], s1send.at[n, step - 1], s1recv.at[n, step - 1],
                                 back(n, step))
        if l == 0:
            phase('turn#l=1')
            turn_qkv(1)
        phase(f'rs_wait#l={l}')
        for n in range(parts):
            cols = slice(n * width, (n + 1) * width)
            sums = [ysend[first_slot(n, 0, g), :, cols] for g in range(4)]
            for step in (1, 3, 2):
                wait(y1.at[n, step - 1], s1recv.at[n, step - 1])
                sums = [t + y1[n, step - 1, g] for g, t in enumerate(sums)]
            for g in range(4):
                yst[n, g] = sums[g]
            for g in (2, 1, 3):
                send(yst.at[n, g], y2.at[n, g - 1], s2send.at[n, g - 1], s2recv.at[n, g - 1], back(n + 1, g))
        phase(f'rs2_wait#l={l}')
        for n in range(parts):
            cols = slice(n * width, (n + 1) * width)
            total = yst[n, 0]
            for g in (1, 3, 2):
                wait(y2.at[n, g - 1], s2recv.at[n, g - 1])
                total = total + y2[n, g - 1]
            hid = bf(f32(hloc[2 * l, :, cols]) + total)
            hloc[2 * l + 1, :, cols] = hid
            if l < layers - 1:
                hrow[pl.ds(i, 1), :, cols] = hid[None]
                for k, s in enumerate(ROW_STEPS):
                    if s[1] == 0 or s[0] == 0:
                        send(hloc.at[2 * l + 1, :, cols], hrow.at[i, :, cols], asend.at[k], arecv.at[k], row_dev(*s))
        if l == 0:
            g_send(1, 1)
        phase(f'drain#l={l}')
        for k in range(len(PLANE_STEPS)):
            wait(cs.at[0], csend.at[k])
        for dz in range(NZ):
            @pl.when(z + dz < NZ)
            def _():
                for dy in range(NY):
                    if dz or dy:
                        wait(kvs.at[0], kvsend.at[dz, dy])
        for dy in (1, 2, 3):
            wait(qs.at[0], qsend.at[dy])
            for n in range(parts):
                wait(y1.at[n, dy - 1], s1send.at[n, dy - 1])
                wait(yst.at[n, dy], s2send.at[n, dy - 1])
        for k in range(COL - 1):
            wait(hloc.at[2 * l], hsend.at[k])
    phase('end')
    for l in range(layers):
        g_drain(l, 0)
        g_drain(l, 1)
    out_ref[...] = bf(norm_rows(f32(hloc[2 * layers - 1]), f32(gfin_ref[...])[None]))
    phase()


def solution(mesh):
    def device_fn(hidden_in, lengths, attn_norm, w_query, w_key, w_value, w_out, mlp_norm, w_gate, w_up, w_down, final_norm):
        batch, tok, d_model = hidden_in.shape
        layers, _, heads, head_dim = w_query.shape
        units = w_gate.shape[2]
        half = head_dim // 2
        freq = ROPE_BASE ** (-2.0 * np.arange(half, dtype=np.float32) / head_dim)
        freq = jnp.asarray(np.tile(freq.astype(np.float32), 4)[None])

        def by_rows(w):
            return jnp.transpose(w, (0, 2, 3, 1)).reshape(layers, heads * head_dim, d_model)

        part = heads // ROW
        wide = 2 * head_dim
        dma = pltpu.SemaphoreType.DMA
        b16 = jnp.bfloat16
        hbm = pl.BlockSpec(memory_space=pl.ANY)
        rtok = ROW * tok
        out = pl.pallas_call(
            kernel,
            name='prefill',
            out_shape=pltpu.VMEM((tok, d_model), b16),
            in_specs=[hbm, pl.BlockSpec(memory_space=pltpu.HBM)] + [hbm] * 11,
            out_specs=pl.BlockSpec(memory_space=pltpu.VMEM),
            scratch_shapes=[
                pltpu.VMEM((d_model, part * wide), b16),
                pltpu.VMEM((d_model, part * head_dim), b16),
                pltpu.VMEM((2, d_model, ROW * units), b16),
                pltpu.VMEM((tok, d_model), b16),
                pltpu.SMEM((1,), jnp.int32),
                pltpu.VMEM((layers, d_model), b16),
                pltpu.VMEM((layers, d_model), b16),
                pltpu.VMEM((d_model,), b16),
                pltpu.VMEM((1, 4 * half), jnp.float32),
                pltpu.VMEM((ROW, tok, d_model), b16),
                pltpu.VMEM((layers, part * head_dim, d_model), b16),
                pltpu.VMEM((layers, part, wide, d_model), b16),
                pltpu.VMEM((layers, heads * head_dim, d_model), b16),
                pltpu.VMEM((layers, ROW, 3, units, d_model), b16),
                pltpu.VMEM((part, rtok, wide), b16),
                pltpu.VMEM((COL, rtok, wide), b16),
                pltpu.VMEM((part, rtok, wide), b16),
                pltpu.VMEM((NY, rtok, wide), b16),
                pltpu.VMEM((NY * ROW, tok, wide), b16),
                pltpu.VMEM((NY * ROW, tok, wide), b16),
                pltpu.VMEM((2 * layers, tok, d_model), b16),
                pltpu.VMEM((COL, tok, d_model), b16),
                pltpu.VMEM((COL * tok, d_model), b16),
                pltpu.VMEM((2, ROW // 2 * COL * tok, ROW // 2 * units), b16),
                pltpu.VMEM((COL, tok, d_model), jnp.float32),
                pltpu.VMEM((4, 3, 4, tok, d_model // 4), jnp.float32),
                pltpu.VMEM((4, 4, tok, d_model // 4), jnp.float32),
                pltpu.VMEM((4, 3, tok, d_model // 4), jnp.float32),
                dma((6,)), dma((layers, 2 * part + 1)), dma((layers,)), dma((layers, 3)),
                dma((ROW - 1,)), dma((ROW - 1,)),
                dma((NZ, NY)), dma((NZ, NY)), dma((NY,)), dma((NY,)),
                dma((NY * ROW - 1,)), dma((NY * ROW - 1,)),
                dma((COL - 1,)), dma((COL - 1,)),
                dma((4, 3)), dma((4, 3)), dma((4, 3)), dma((4, 3)),
                dma((layers, 2, 9)), dma((layers, 2, 9)),
            ],
            compiler_params=pltpu.CompilerParams(collective_id=0, has_side_effects=True, vmem_limit_bytes=60 * 1024 * 1024),
        )(hidden_in.reshape(tok, d_model), lengths, attn_norm, mlp_norm, final_norm, freq,
          by_rows(w_query), by_rows(w_key), by_rows(w_value), w_out.reshape(layers, heads * head_dim, d_model),
          jnp.transpose(w_gate, (0, 2, 1)), jnp.transpose(w_up, (0, 2, 1)), w_down)
        return out.reshape(batch, tok, d_model)

    seq_part = P(None, 'tp', None)
    in_specs = (seq_part, P(), P(), P(), P(), P(), P(), P(), P(None, None, 'tp'), P(None, None, 'tp'), P(None, 'tp', None), P())
    return jax.shard_map(device_fn, mesh=mesh, in_specs=in_specs, out_specs=seq_part, check_vma=False)
```

```python
import functools

import jax
import jax.numpy as jnp
import numpy as np
from jax import lax
from jax.experimental import pallas as pl
from jax.experimental.pallas import tpu as pltpu
from jax.sharding import PartitionSpec as P

NORM_EPS = 1e-5
ROPE_BASE = 500000.0
MESH = pl.DeviceIdType.MESH
NX, NY, NZ = 4, 4, 4
ROW = 2 * NX
COL = NY * NZ


def far(d):
    return min(d, NX - d)


ROW_STEPS = sorted(((dx, dc) for dx in range(NX) for dc in range(2) if dx or dc), key=lambda s: (-far(s[0]), -s[1]))
COL_STEPS = sorted(((dz, dy) for dz in range(NZ) for dy in range(NY) if dz or dy),
                   key=lambda s: (s[1] % 2, s[0] > 0, s[1] * (1 - s[1] % 2), far(s[0]), s))
SLOT = {s: k for k, s in enumerate([(0, 0)] + COL_STEPS)}
PLANE_STEPS = sorted(((dy, dx, dc) for dy in range(NY) for dx in range(NX) for dc in range(2) if dy or dx or dc),
                     key=lambda s: -far(s[0]) - far(s[1]))


class Phases:
    def __init__(self):
        self.open = None

    def __call__(self, name=None):
        if self.open is not None:
            self.open.__exit__(None, None, None)
        self.open = jax.named_scope(name) if name else None
        if name:
            self.open.__enter__()


def bf(v):
    return v.astype(jnp.bfloat16)


def f32(v):
    return v.astype(jnp.float32)


def dot_nt(a, b):
    return lax.dot_general(a, b, (((1,), (1,)), ((), ())), preferred_element_type=jnp.float32)


def norm_rows(h, gain):
    inv = lax.rsqrt(jnp.mean(h * h, axis=-1, keepdims=True) + NORM_EPS)
    return h * inv * gain


def kernel(h_in, len_in, gattn_in, gmlp_in, gfin_in, freq_in, wq_ref, wk_ref, wv_ref, wo_ref, wg_ref, wu_ref, wd_ref,
           out_ref,
           wkv_t, wq_t, wgu_t, h_ref, len_ref, gattn_ref, gmlp_ref, gfin_ref, freq_ref, hrow, wq_s, wkv_s, wo_s, wm, kvs, kvbuf, qs, qbuf, cs, cbuf, hloc, hcol, zs, acts, ysend, y1, yst, y2,
           isem, lsem, wosem, msem, asend, arecv, kvsend, kvrecv, qsend, qrecv, csend, crecv, hsend, hrecv, s1send, s1recv, s2send, s2recv, gsend, grecv):
    phase = Phases()
    phase('start')
    layers = wo_s.shape[0]
    tok, d_model = h_ref.shape
    rtok = ROW * tok
    heads, wide = kvs.shape[0], kvs.shape[2]
    hd = wide // 2
    half = hd // 2
    units = wm.shape[3]
    me = lax.axis_index('tp')
    core = lax.rem(me, 2)
    i = lax.rem(me, ROW)
    x = i // 2
    r = me // ROW
    y = lax.rem(r, NY)
    z = r // NY

    def row_id(dx, dc):
        return 2 * lax.rem(x + (dx + NX) % NX, NX) + (1 - core if dc else core)

    def row_dev(dx, dc):
        return (r * ROW + row_id(dx, dc),)

    def y_at(dy):
        return lax.rem(y + (dy + NY) % NY, NY)

    def plane_dev(dy, dx, dc):
        return ((z * NY + y_at(dy)) * ROW + row_id(dx, dc),)

    def col_dev(dz, dy):
        return ((NY * lax.rem(z + (dz + NZ) % NZ, NZ) + y_at(dy)) * ROW + i,)

    def first_slot(n, step, g):
        return SLOT[(g, step) if n % 2 == 0 else (step, g)]

    def back(n, step):
        return col_dev(0, -step) if n % 2 == 0 else col_dev(-step, 0)

    def send(src, dst, ssem, rsem, dev):
        pltpu.make_async_remote_copy(src_ref=src, dst_ref=dst, send_sem=ssem, recv_sem=rsem, device_id=dev,
                                     device_id_type=MESH).start()

    def wait(ref, sem):
        pltpu.make_async_copy(ref, ref, sem).wait()

    def load(src, dst, sem):
        c = pltpu.make_async_copy(src, dst, sem)
        c.start()
        return c

    def load_qkv(l):
        base = i * (heads * hd)
        got = []
        for j in range(heads):
            rows = pl.ds(base + j * hd, hd)
            got.append(load(wk_ref.at[l, rows], wkv_s.at[l, j, 0:hd], lsem.at[l, 2 * j]))
            got.append(load(wv_ref.at[l, rows], wkv_s.at[l, j, hd:wide], lsem.at[l, 2 * j + 1]))
        got.append(load(wq_ref.at[l, pl.ds(base, heads * hd)], wq_s.at[l], lsem.at[l, 2 * heads]))
        return got

    def load_mlp(l):
        return [load(w.at[l], wm.at[l, i, k], msem.at[l, k]) for k, w in enumerate((wg_ref, wu_ref, wd_ref))]

    h_load = load(h_in, h_ref, isem.at[0])
    barrier = pltpu.get_barrier_semaphore()
    partners = [plane_dev(*s) for s in PLANE_STEPS] + [col_dev(*s) for s in COL_STEPS if s[0]]
    for dev in partners:
        pl.semaphore_signal(barrier, inc=1, device_id=dev, device_id_type=MESH)
    inputs = [load(src, dst, isem.at[k + 1]) for k, (src, dst) in enumerate((
        (freq_in, freq_ref), (gattn_in, gattn_ref), (gmlp_in, gmlp_ref), (gfin_in, gfin_ref),
        (len_in, len_ref)))]
    mlp_loads = [load_mlp(0)]
    qkv_loads = [load_qkv(0)]
    wo_loads = [load(wo_ref.at[0], wo_s.at[0], wosem.at[0])]
    mlp_loads.append(load_mlp(1))
    qkv_loads.append(load_qkv(1))
    wo_loads.append(load(wo_ref.at[1], wo_s.at[1], wosem.at[1]))
    for zz in range(1, NZ):
        @pl.when(zz > z)
        def _():
            kvbuf[zz * NY:(zz + 1) * NY] = jnp.zeros((NY, rtok, wide), kvbuf.dtype)
    phase('barrier')
    h_load.wait()
    pl.semaphore_wait(barrier, len(partners))

    hu = units // 2
    spans = (pl.ds(0, 2), pl.ds(2, 1))
    low, high = pl.ds(0, hu), pl.ds(hu, hu)

    def blk(l, p, dx, dc, rows=None):
        if rows is None:
            return wm.at[l, row_id(dx, dc), spans[p]]
        return wm.at[l, row_id(dx, dc), spans[p], rows]

    def g_push(l, p, k, ref, dx, dc):
        send(ref, ref, gsend.at[l, p, k], grecv.at[l, p, k], row_dev(dx, dc))

    def g_send(l, p):
        for c in (mlp_loads[l][:2], mlp_loads[l][2:])[p]:
            c.wait()
        own = blk(l, p, 0, 0)
        g_push(l, p, 1, own, 1, 0)
        g_push(l, p, 2, own, -1, 0)
        g_push(l, p, 0, own, 0, 1)

    def g_fwd(l, p):
        wait(blk(l, p, -1, 0), grecv.at[l, p, 1])
        g_push(l, p, 3, blk(l, p, -1, 0, low), 1, 0)
        wait(blk(l, p, 1, 0), grecv.at[l, p, 2])
        g_push(l, p, 4, blk(l, p, 1, 0, high), -1, 0)
        g_push(l, p, 5, blk(l, p, -1, 0), 0, 1)
        g_push(l, p, 6, blk(l, p, 1, 0), 0, 1)

    def g_fwd2(l, p):
        for k, rows in enumerate((low, high)):
            wait(blk(l, p, 2, 0, rows), grecv.at[l, p, 3 + k])
            g_push(l, p, 7 + k, blk(l, p, 2, 0, rows), 0, 1)

    def g_done(l, p):
        wait(blk(l, p, 0, 1), grecv.at[l, p, 0])
        wait(blk(l, p, -1, 1), grecv.at[l, p, 5])
        wait(blk(l, p, 1, 1), grecv.at[l, p, 6])
        for k, rows in enumerate((low, high)):
            wait(blk(l, p, 2, 1, rows), grecv.at[l, p, 7 + k])

    def g_drain(l, p):
        for k in (0, 1, 2, 5, 6):
            wait(blk(l, p, 0, 0), gsend.at[l, p, k])
        for k in (3, 4, 7, 8):
            wait(blk(l, p, 0, 0, low), gsend.at[l, p, k])


    def turned(p, c, s):
        swapped = jnp.where(lax.rem(lane, hd) < half, pltpu.roll(p, wide - half, 1), pltpu.roll(p, half, 1))
        return p * c + swapped * s

    def turn_qkv(l):
        for c in qkv_loads[l]:
            c.wait()
        for j in range(heads):
            wkv_t[:, j * wide:(j + 1) * wide] = wkv_s[l, j].T
        for j in range(heads // 2):
            wq_t[:, j * wide:(j + 1) * wide] = wq_s[l, j * wide:(j + 1) * wide].T

    def turn_mlp(l):
        for j in range(0, ROW, 2):
            for k in range(2):
                wgu_t[k, :, j * units:(j + 2) * units] = wm[l, j:j + 2, k].reshape(2 * units, d_model).T

    for l in range(layers):
        phase(f'row_h#l={l}')
        if l == 0:
            for k, s in enumerate(ROW_STEPS):
                if s[1] == 0 or s[0] == 0:
                    send(h_ref, hrow.at[i], asend.at[k], arecv.at[k], row_dev(*s))
            g_send(0, 0)
            hrow[pl.ds(i, 1)] = h_ref[...][None]
            for c in inputs:
                c.wait()
            lane = lax.broadcasted_iota(jnp.int32, (1, wide), 1)
            pos = f32(r * rtok + lax.broadcasted_iota(jnp.int32, (rtok, 1), 0))
            angles = pos * freq_ref[...]
            cos_tab = jnp.cos(angles)
            sin_tab = jnp.sin(angles)
            sin_tab = jnp.where(lax.rem(lane, hd) < half, -sin_tab, sin_tab)
            phase('turn#l=0')
            turn_qkv(0)
            phase('row_wait#l=0')
        if True:
            for dx in (1, 3, 2):
                wait(hrow.at[row_id(-dx, 0)], arecv.at[ROW_STEPS.index((dx, 0))])
                k = ROW_STEPS.index((dx, 1))
                send(hrow.at[row_id(-dx, 0)], hrow.at[row_id(-dx, 0)], asend.at[k], arecv.at[k], row_dev(0, 1))
        for k, (dx, dc) in enumerate(ROW_STEPS):
            if dc:
                wait(hrow.at[row_id(-dx, dc)], arecv.at[k])
        length = len_ref[0]
        phase(f'qkv#l={l}')
        g_attn = f32(gattn_ref[...])[l:l + 1]
        g_mlp = f32(gmlp_ref[...])[l:l + 1]
        zs[0:rtok] = bf(norm_rows(f32(hrow[...]).reshape(rtok, d_model), g_attn))
        kv = jnp.dot(zs[0:rtok], wkv_t[...], preferred_element_type=jnp.float32)
        for j in range(heads):
            p = kv[:, j * wide:(j + 1) * wide]
            kvs[j] = bf(jnp.where(lane < hd, turned(p, cos_tab, sin_tab), p))
        for dz in (3, 2, 1, 0):
            @pl.when(z + dz < NZ)
            def _():
                for dy in (2, 1, 3, 0):
                    if dz or dy:
                        send(kvs.at[y_at(dy)], kvbuf.at[r], kvsend.at[dz, dy], kvrecv.at[dz, dy], col_dev(dz, dy))
        kvbuf[pl.ds(r, 1)] = kvs[pl.ds(y, 1)]
        q = jnp.dot(zs[0:rtok], wq_t[...], preferred_element_type=jnp.float32)
        for j in range(0, heads, 2):
            pair = turned(q[:, j * hd:(j + 2) * hd], cos_tab, sin_tab)
            qs[j] = bf(jnp.where(lane < hd, pair, 0.0))
            qs[j + 1] = bf(jnp.where(lane < hd, pltpu.roll(pair, hd, 1), 0.0))
        for dy in (2, 1, 3):
            send(qs.at[y_at(dy)], qbuf.at[y], qsend.at[dy], qrecv.at[dy], col_dev(0, dy))
        qbuf[pl.ds(y, 1)] = qs[pl.ds(y, 1)]
        phase(f'kv_wait#l={l}')
        for dy in (1, 3, 2):
            wait(qbuf.at[y_at(-dy)], qrecv.at[dy])
        for dz in range(NZ):
            @pl.when(z - dz >= 0)
            def _():
                for dy in range(NY):
                    if dz or dy:
                        wait(kvbuf.at[(z - dz) * NY + y_at(-dy)], kvrecv.at[dz, dy])
        for k in range(ROW - 1):
            wait(h_ref, asend.at[k])
        phase(f'attn#l={l}')
        keys = COL * rtok
        quer = NY * rtok
        kv_all = kvbuf[...].reshape(keys, wide)
        scores = dot_nt(qbuf[...].reshape(quer, wide), kv_all) * hd ** -0.5
        k_pos = lax.broadcasted_iota(jnp.int32, (1, keys), 1)
        limit = jnp.minimum(z * quer + 1 + lax.broadcasted_iota(jnp.int32, (quer, 1), 0), length)
        scores = jnp.where(k_pos < limit, scores, -1e30)
        e = jnp.exp(scores - jnp.max(scores, axis=-1, keepdims=True))
        probs = bf(e * (1.0 / jnp.sum(e, axis=-1, keepdims=True)))
        pv = jnp.dot(probs, kv_all, preferred_element_type=jnp.float32)
        ctx = jnp.where(lax.rem(y, 2) == 0, pltpu.roll(pv, hd, 1), pv)
        cs[...] = bf(ctx.reshape(NY * ROW, tok, wide))
        phase(f'ctx#l={l}')
        slot = ROW * y + i
        for k, (dy, dx, dc) in enumerate(PLANE_STEPS):
            send(cs.at[ROW * y_at(dy) + row_id(dx, dc)], cbuf.at[slot], csend.at[k], crecv.at[k], plane_dev(dy, dx, dc))
        cbuf[pl.ds(slot, 1)] = cs[pl.ds(slot, 1)]
        phase(f'g_b#l={l}')
        if l == 0:
            g_send(0, 1)
            g_fwd(0, 0)
        else:
            g_fwd(1, 0)
            g_fwd(1, 1)
        wo_loads[l].wait()
        attn_out = jnp.zeros((tok, d_model), jnp.float32)
        for step in (0, 1, 3, 2):
            phase(f'ctx_wait#l={l}#s={step}')
            for k, (dy, dx, dc) in enumerate(PLANE_STEPS):
                if dx == step:
                    wait(cbuf.at[ROW * y_at(-dy) + row_id(-dx, dc)], crecv.at[k])
            phase(f'out#l={l}#s={step}')
            chip = lax.rem(x - step + NX, NX)
            pieces = []
            for c in range(2):
                for j in range(0, heads, 2):
                    pieces.append(jnp.where(lane < hd, cbuf[j * ROW + 2 * chip + c], cbuf[(j + 1) * ROW + 2 * chip + c]))
            ctx_chip = jnp.concatenate(pieces, axis=1)
            rows = pl.ds(pl.multiple_of(chip * (2 * heads * hd), 2 * heads * hd), 2 * heads * hd)
            if step != 2:
                attn_out = attn_out + jnp.dot(ctx_chip, wo_s[l, rows, :], preferred_element_type=jnp.float32)
        for n in range(2):
            cols = slice(n * (d_model // 2), (n + 1) * (d_model // 2))
            part_out = attn_out[:, cols] + jnp.dot(ctx_chip, wo_s[l, rows, cols], preferred_element_type=jnp.float32)
            hid = bf(f32(h_ref[:, cols] if l == 0 else hloc[2 * l - 1, :, cols]) + part_out)
            hloc[2 * l, :, cols] = hid
            hcol[0, :, cols] = hid
            for k, s in enumerate(COL_STEPS[:COL // 2 - 1]):
                send(hloc.at[2 * l, :, cols], hcol.at[k + 1, :, cols], hsend.at[k], hrecv.at[k], col_dev(*s))
        for k, s in list(enumerate(COL_STEPS))[COL // 2 - 1:]:
            send(hloc.at[2 * l], hcol.at[k + 1], hsend.at[k], hrecv.at[k], col_dev(*s))
        phase(f'col_h#l={l}')
        if l == 0:
            g_fwd(0, 1)
        g_fwd2(l, 0)
        if l == 1:
            g_done(1, 0)
            phase('turn_mlp')
            turn_mlp(1)
            phase(f'col_h2#l={l}')
            g_fwd2(1, 1)
        grp = ROW // 2
        ulane = lax.broadcasted_iota(jnp.int32, (1, grp * units), 1) // units
        parts = 4
        width = d_model // parts
        halves = 1 if l == 0 else 2
        slots = COL // halves
        m = slots * tok
        for part in range(halves):
            phase(f'col_h_wait#l={l}#p={part}')
            for k in range(part * slots, (part + 1) * slots):
                if k:
                    wait(hcol.at[k], hrecv.at[k - 1])
            mine = slice(part * slots, (part + 1) * slots)
            zs[0:m] = bf(norm_rows(f32(hcol[mine]).reshape(m, d_model), g_mlp))
            if l == 0:
                phase(f'g_done#l={l}')
                g_done(0, 0)
            phase(f'mlp_up#l={l}#p={part}')
            for b in range(2):
                if l == 0:
                    gate = dot_nt(zs[0:m], wm[l, b * grp:(b + 1) * grp, 0].reshape(grp * units, d_model))
                    up = dot_nt(zs[0:m], wm[l, b * grp:(b + 1) * grp, 1].reshape(grp * units, d_model))
                else:
                    these = slice(b * grp * units, (b + 1) * grp * units)
                    gate = jnp.dot(zs[0:m], wgu_t[0, :, these], preferred_element_type=jnp.float32)
                    up = jnp.dot(zs[0:m], wgu_t[1, :, these], preferred_element_type=jnp.float32)
                act = bf(gate * (1.0 / (1.0 + jnp.exp(-gate))) * up)
                for j in range(grp):
                    acts[b, j * m:(j + 1) * m] = jnp.where(ulane == j, act, jnp.zeros_like(act))
                if l == 0 and b == 0:
                    phase(f'g_fwd2#l={l}')
                    g_fwd2(0, 1)
                    phase(f'mlp_up2#l={l}#p={part}')
            if part == 0:
                phase(f'g_done2#l={l}')
                if l == 0:
                    g_send(1, 0)
                g_done(l, 1)
            phase(f'mlp_down#l={l}#p={part}')
            for n in range(parts):
                cols = slice(n * width, (n + 1) * width)
                total = jnp.zeros((m, width), jnp.float32)
                for b in range(2):
                    wd = wm[l, b * grp:(b + 1) * grp, 2, :, cols].reshape(grp * units, width)
                    prod = jnp.dot(acts[b, 0:grp * m], wd, preferred_element_type=jnp.float32)
                    for j in range(grp):
                        total = total + f32(bf(prod[j * m:(j + 1) * m]))
                ysend[mine, :, cols] = total.reshape(slots, tok, width)
                for step in (2, 1, 3):
                    for g in range(4):
                        k = first_slot(n, step, g)
                        if part * slots <= k < (part + 1) * slots:
                            send(ysend.at[k, :, cols], y1.at[n, step - 1, g], s1send.at[n, step - 1], s1recv.at[n, step - 1],
                                 back(n, step))
        if l == 0:
            phase('turn#l=1')
            turn_qkv(1)
        phase(f'rs_wait#l={l}')
        for k in range(len(PLANE_STEPS)):
            wait(cs.at[0], csend.at[k])
        for dz in range(NZ):
            @pl.when(z + dz < NZ)
            def _():
                for dy in range(NY):
                    if dz or dy:
                        wait(kvs.at[0], kvsend.at[dz, dy])
        for dy in (1, 2, 3):
            wait(qs.at[0], qsend.at[dy])
        for k in range(COL - 1):
            wait(hloc.at[2 * l], hsend.at[k])
        for n in range(parts):
            cols = slice(n * width, (n + 1) * width)
            sums = [ysend[first_slot(n, 0, g), :, cols] for g in range(4)]
            for step in (1, 3, 2):
                wait(y1.at[n, step - 1], s1recv.at[n, step - 1])
                sums = [t + y1[n, step - 1, g] for g, t in enumerate(sums)]
            for g in range(4):
                yst[n, g] = sums[g]
            for g in (2, 1, 3):
                send(yst.at[n, g], y2.at[n, g - 1], s2send.at[n, g - 1], s2recv.at[n, g - 1], back(n + 1, g))
        phase(f'rs2_wait#l={l}')
        for n in range(parts):
            cols = slice(n * width, (n + 1) * width)
            total = yst[n, 0]
            for g in (1, 3, 2):
                wait(y2.at[n, g - 1], s2recv.at[n, g - 1])
                total = total + y2[n, g - 1]
            hid = bf(f32(hloc[2 * l, :, cols]) + total)
            hloc[2 * l + 1, :, cols] = hid
            if l < layers - 1:
                hrow[pl.ds(i, 1), :, cols] = hid[None]
                for k, s in enumerate(ROW_STEPS):
                    if s[1] == 0 or s[0] == 0:
                        send(hloc.at[2 * l + 1, :, cols], hrow.at[i, :, cols], asend.at[k], arecv.at[k], row_dev(*s))
        if l == 0:
            g_send(1, 1)
        phase(f'drain#l={l}')
        for g in range(3):
            for n in range(parts):
                wait(y1.at[n, g], s1send.at[n, g])
                wait(yst.at[n, g + 1], s2send.at[n, g])
    phase('end')
    for l in range(layers):
        g_drain(l, 0)
        g_drain(l, 1)
    out_ref[...] = bf(norm_rows(f32(hloc[2 * layers - 1]), f32(gfin_ref[...])[None]))
    phase()


def solution(mesh):
    def device_fn(hidden_in, lengths, attn_norm, w_query, w_key, w_value, w_out, mlp_norm, w_gate, w_up, w_down, final_norm):
        batch, tok, d_model = hidden_in.shape
        layers, _, heads, head_dim = w_query.shape
        units = w_gate.shape[2]
        half = head_dim // 2
        freq = ROPE_BASE ** (-2.0 * np.arange(half, dtype=np.float32) / head_dim)
        freq = jnp.asarray(np.tile(freq.astype(np.float32), 4)[None])

        def by_rows(w):
            return jnp.transpose(w, (0, 2, 3, 1)).reshape(layers, heads * head_dim, d_model)

        part = heads // ROW
        wide = 2 * head_dim
        dma = pltpu.SemaphoreType.DMA
        b16 = jnp.bfloat16
        hbm = pl.BlockSpec(memory_space=pl.ANY)
        rtok = ROW * tok
        out = pl.pallas_call(
            kernel,
            name='prefill',
            out_shape=pltpu.VMEM((tok, d_model), b16),
            in_specs=[hbm, pl.BlockSpec(memory_space=pltpu.HBM)] + [hbm] * 11,
            out_specs=pl.BlockSpec(memory_space=pltpu.VMEM),
            scratch_shapes=[
                pltpu.VMEM((d_model, part * wide), b16),
                pltpu.VMEM((d_model, part * head_dim), b16),
                pltpu.VMEM((2, d_model, ROW * units), b16),
                pltpu.VMEM((tok, d_model), b16),
                pltpu.SMEM((1,), jnp.int32),
                pltpu.VMEM((layers, d_model), b16),
                pltpu.VMEM((layers, d_model), b16),
                pltpu.VMEM((d_model,), b16),
                pltpu.VMEM((1, 4 * half), jnp.float32),
                pltpu.VMEM((ROW, tok, d_model), b16),
                pltpu.VMEM((layers, part * head_dim, d_model), b16),
                pltpu.VMEM((layers, part, wide, d_model), b16),
                pltpu.VMEM((layers, heads * head_dim, d_model), b16),
                pltpu.VMEM((layers, ROW, 3, units, d_model), b16),
                pltpu.VMEM((part, rtok, wide), b16),
                pltpu.VMEM((COL, rtok, wide), b16),
                pltpu.VMEM((part, rtok, wide), b16),
                pltpu.VMEM((NY, rtok, wide), b16),
                pltpu.VMEM((NY * ROW, tok, wide), b16),
                pltpu.VMEM((NY * ROW, tok, wide), b16),
                pltpu.VMEM((2 * layers, tok, d_model), b16),
                pltpu.VMEM((COL, tok, d_model), b16),
                pltpu.VMEM((COL * tok, d_model), b16),
                pltpu.VMEM((2, ROW // 2 * COL * tok, ROW // 2 * units), b16),
                pltpu.VMEM((COL, tok, d_model), jnp.float32),
                pltpu.VMEM((4, 3, 4, tok, d_model // 4), jnp.float32),
                pltpu.VMEM((4, 4, tok, d_model // 4), jnp.float32),
                pltpu.VMEM((4, 3, tok, d_model // 4), jnp.float32),
                dma((6,)), dma((layers, 2 * part + 1)), dma((layers,)), dma((layers, 3)),
                dma((ROW - 1,)), dma((ROW - 1,)),
                dma((NZ, NY)), dma((NZ, NY)), dma((NY,)), dma((NY,)),
                dma((NY * ROW - 1,)), dma((NY * ROW - 1,)),
                dma((COL - 1,)), dma((COL - 1,)),
                dma((4, 3)), dma((4, 3)), dma((4, 3)), dma((4, 3)),
                dma((layers, 2, 9)), dma((layers, 2, 9)),
            ],
            compiler_params=pltpu.CompilerParams(collective_id=0, has_side_effects=True, vmem_limit_bytes=60 * 1024 * 1024),
        )(hidden_in.reshape(tok, d_model), lengths, attn_norm, mlp_norm, final_norm, freq,
          by_rows(w_query), by_rows(w_key), by_rows(w_value), w_out.reshape(layers, heads * head_dim, d_model),
          jnp.transpose(w_gate, (0, 2, 1)), jnp.transpose(w_up, (0, 2, 1)), w_down)
        return out.reshape(batch, tok, d_model)

    seq_part = P(None, 'tp', None)
    in_specs = (seq_part, P(), P(), P(), P(), P(), P(), P(), P(None, None, 'tp'), P(None, None, 'tp'), P(None, 'tp', None), P())
    return jax.shard_map(device_fn, mesh=mesh, in_specs=in_specs, out_specs=seq_part, check_vma=False)
```
